768 devices in a mesh: ctx: 24 (over z, x_hi), tp: 32 (over x_lo, y, core).
Axes of the slice: x: 4 (x_hi: 2, x_lo: 2; x = x_hi * 2 + x_lo), y: 8, z: 12, core: 2. Of those that a mesh axis runs over, the one named last changes fastest.
Arguments:
- q_nope: bfloat16 [3072, 16384], P('ctx', 'tp'), may hold values from -5 to 5
- q_rope: bfloat16 [3072, 8192], P('ctx', 'tp'), may hold values from -128 to 128
- cache_latent: bfloat16 [768, 576], P('ctx'), may hold values from -4 to 4
- group_latent: bfloat16 [3072, 576], P('ctx'), may hold values from -4 to 4
- offset: int32 [1], replicated, may hold values from 768 to 1535
- counts: int32 [24], replicated, may hold values from 1 to 32, as said below
- up_key: bfloat16 [128, 128, 512], P('tp'), may hold values from -0.5 to 0.5
- up_value: bfloat16 [128, 512, 128], P('tp'), may hold values from -0.25 to 0.25
- out_weight: bfloat16 [16384, 7168], P('tp'), may hold values from -0.09375 to 0.09375
Outputs:
- attn_out: bfloat16 [3072, 7168], P('ctx', 'tp')
The draws below stay inside these ranges and needn't reach their ends.
Inputs may be any that keep to these rules, and one draw needn't show every extreme that they name: counts[c] cache slots of context index c are live, the first ones; some index has all 32 live in every draw. `offset`: at least the number of cache slots in all.
All inputs are finite; a program needn't handle non-finite values.
Results may differ from the reference program's by a relative error of at most 0.025.
Values may be sent and summed in bfloat16 or wider, within the bound.
A program may use at most 64 MiB of HBM per device.

```python
import jax
import jax.numpy as jnp
from jax import lax

D = 7168
HEADS = 128
LATENT = 512
ROPE = 64
NOPE = 128
VDIM = 128
TOK_DEV = 128
CACHE_DEV = 32
TOKENS = 3072
CACHE = 768
N_CTX = 24


def draw_group_latent(key, part):
    values = jnp.clip(jax.random.normal(jax.random.fold_in(key, 5), (TOKENS, LATENT + ROPE), jnp.float32), -4.0, 4.0)
    return values.astype(jnp.bfloat16)


def draw_q_rope(key, part):
    values = jnp.clip(jax.random.normal(jax.random.fold_in(key, 6), (TOKENS, HEADS * ROPE), jnp.float32), -4.0, 4.0)
    return values.astype(jnp.bfloat16)


def draw_counts(key, part):
    values = jax.random.randint(jax.random.fold_in(key, 7), (N_CTX,), 1, CACHE_DEV + 1)
    full_index = jax.random.randint(jax.random.fold_in(key, 8), (), 0, N_CTX)
    return jnp.where(jnp.arange(N_CTX) == full_index, CACHE_DEV, values).astype(jnp.int32)


def with_spikes(values, key, source, target, parts, factor):
    owner, partner = [(jnp.arange(values.shape[position]) // (values.shape[position] // parts)).reshape([-1 if axis == position else 1 for axis in range(values.ndim)]) for position in (source, target)]
    chosen = jax.random.permutation(key, parts)[partner]
    strong = (owner == chosen) | (owner == (partner + parts // 2) % parts)
    return jnp.where(strong, factor * values, values)


def block_scale(rng, extent, split, smallest, high):
    loudness, own = 1.0, jax.random.fold_in(rng, 6)
    for position, shards_of in split:
        heights = jnp.exp(jax.random.uniform(jax.random.fold_in(own, position), (shards_of,), jnp.float32, smallest / len(split), high / len(split)))
        loudness = loudness * jnp.repeat(heights, extent[position] // shards_of).reshape([-1 if axis == position else 1 for axis in range(len(extent))])
    return loudness


def scatter_about(stream_key, extent, spread, limit, shards=(), kind=jnp.bfloat16):
    result = jax.random.normal(stream_key, extent, jnp.float32) * spread
    if len(shards) > 0:
        result = block_scale(stream_key, extent, shards, -0.22, 0.18) * result
    return jnp.clip(result, min=-limit, max=limit).astype(kind)


def bell_draw_with(rng, dims, spread, limit, shards, heavy, kind=jnp.bfloat16):
    values = spread * jax.random.normal(rng, dims, jnp.float32)
    if shards:
        values = values * block_scale(rng, dims, shards, -0.22, 0.18)
    return jnp.clip(with_spikes(values, jax.random.fold_in(rng, 3), *heavy), -limit, limit).astype(kind)


def setup_inputs(seed: int = 0) -> dict:
    splits = jax.random.split(jax.random.key(seed), 10)
    q_nope = scatter_about(splits[0], (TOKENS, HEADS * NOPE), 1.0, 5.0, ((0, 24), (1, 32)))
    q_rope = draw_q_rope(jax.random.fold_in(splits[9], 71), 0)
    cache_latent = scatter_about(splits[2], (CACHE, LATENT + ROPE), 1.0, 4.0, ((0, 24),))
    group_latent = draw_group_latent(jax.random.fold_in(splits[9], 71), 0)
    offset = jax.random.randint(splits[4], (1,), N_CTX * CACHE_DEV, 2 * N_CTX * CACHE_DEV).astype(jnp.int32)
    counts = draw_counts(jax.random.fold_in(splits[9], 71), 0)
    up_key = scatter_about(splits[6], (HEADS, NOPE, LATENT), NOPE ** -0.5, 0.5, ((0, 32),))
    up_value = scatter_about(splits[7], (HEADS, LATENT, VDIM), LATENT ** -0.5, 0.25, ((0, 32),))
    out_weight = bell_draw_with(splits[8], (HEADS * VDIM, D), (HEADS * VDIM) ** -0.5, 0.09375, ((0, 32),), (0, 1, 32, 2.75))
    return dict(q_nope=q_nope, q_rope=q_rope, cache_latent=cache_latent, group_latent=group_latent, offset=offset, counts=counts, up_key=up_key, up_value=up_value, out_weight=out_weight)


def rotate(values, positions):
    half_width = values.shape[-1] // 2
    frequency = 10000.0 ** (-2.0 * jnp.arange(half_width, dtype=jnp.float32) / ROPE)
    angles = positions.astype(jnp.float32)[:, None] * frequency[None, :]
    cosine = jnp.cos(angles)
    sine_part = jnp.sin(angles)
    if values.ndim == 3:
        cosine = cosine[:, None, :]
        sine_part = sine_part[:, None, :]
    front_half = values[..., :half_width].astype(jnp.float32)
    back_half = values[..., half_width:].astype(jnp.float32)
    joined = jnp.concatenate([front_half * cosine - back_half * sine_part, back_half * cosine + front_half * sine_part], -1)
    return joined.astype(jnp.bfloat16)


def reference(q_nope, q_rope, cache_latent, group_latent, offset, counts, up_key, up_value, out_weight):
    positions = offset[0] + jnp.arange(TOKENS, dtype=jnp.int32)
    query_rope = rotate(q_rope.reshape(TOKENS, HEADS, ROPE), positions)
    key_rope = rotate(group_latent[:, LATENT:], positions)
    group_keys = jnp.concatenate([group_latent[:, :LATENT], key_rope], 1)
    span_rows = CACHE_DEV + TOK_DEV
    all_keys = jnp.concatenate([cache_latent.reshape(N_CTX, CACHE_DEV, LATENT + ROPE), group_keys.reshape(N_CTX, TOK_DEV, LATENT + ROPE)], 1)
    all_keys = all_keys.reshape(N_CTX * span_rows, LATENT + ROPE)
    key_index = jnp.arange(N_CTX * span_rows, dtype=jnp.int32)
    key_owner = key_index // span_rows
    key_slot = key_index % span_rows
    is_live = (key_slot < CACHE_DEV) & (key_slot < counts[key_owner])
    group_index = key_owner * TOK_DEV + key_slot - CACHE_DEV
    token_index = jnp.arange(TOKENS, dtype=jnp.int32)
    visible = is_live[None, :] | ((key_slot >= CACHE_DEV)[None, :] & (group_index[None, :] <= token_index[:, None]))
    score_scale = 1.0 / (NOPE + ROPE) ** 0.5
    latent_t = all_keys[:, :LATENT].T
    rope_t = all_keys[:, LATENT:].T
    latent_rows = all_keys[:, :LATENT]
    nope_heads = q_nope.reshape(TOKENS, HEADS, NOPE).transpose(1, 0, 2)
    rope_heads = query_rope.transpose(1, 0, 2)

    def one_head(inputs):
        nope_part, rope_part, key_weight, value_weight = inputs
        query_latent = jnp.dot(nope_part, key_weight, preferred_element_type=jnp.float32).astype(jnp.bfloat16)
        scores = jnp.dot(query_latent, latent_t, preferred_element_type=jnp.float32)
        scores = (scores + jnp.dot(rope_part, rope_t, preferred_element_type=jnp.float32)) * score_scale
        scores = jnp.where(visible, scores, -jnp.inf)
        row_max = jnp.max(scores, axis=1, keepdims=True)
        expos = jnp.exp(scores - row_max)
        row_sum = jnp.sum(expos, axis=1, keepdims=True)
        mixed = jnp.dot(expos.astype(jnp.bfloat16), latent_rows, preferred_element_type=jnp.float32) / row_sum
        attended = mixed.astype(jnp.bfloat16)
        return jnp.dot(attended, value_weight, preferred_element_type=jnp.float32).astype(jnp.bfloat16)

    head_out = lax.map(one_head, (nope_heads, rope_heads, up_key, up_value))
    joined = head_out.transpose(1, 0, 2).reshape(TOKENS, HEADS * VDIM)
    return jnp.dot(joined, out_weight, preferred_element_type=jnp.float32).astype(jnp.bfloat16)
```

```python
import math

import jax
import jax.numpy as jnp
import numpy as np
from jax import lax
from jax.experimental import pallas as pl
from jax.experimental.pallas import tpu as pltpu
from jax.sharding import PartitionSpec as P

LATENT = 512
ROPE = 64
NOPE = 128
VDIM = 128
WIDE = 640
NZ = 12
NY = 8
TOK = 128
CACHED = 32
SPAN = 160
HEADS = 4
ROWS = TOK * HEADS
CHUNK = 4 * SPAN
WIN = 512
NEG = -1e30
SCALE = math.log2(math.e) / math.sqrt(NOPE + ROPE)
GROUP = 256
MESH = pl.DeviceIdType.MESH
F32 = jnp.float32
BF16 = jnp.bfloat16


def slot(i, s, o):
    if isinstance(i, int):
        if i == 0:
            return 5 * CHUNK + o * SPAN
        if i == 6:
            return 5 * CHUNK + 2 * SPAN + o * SPAN
    return (i - 1) * CHUNK + s * 2 * SPAN + o * SPAN


def rows_at(ref, start, size):
    if not isinstance(start, int):
        start = pl.multiple_of(start, 16)
    return ref.at[pl.ds(start, size), :]


def kernel(
    offset_ref, counts_ref, freq_ref, q_nope_hbm, q_rope_hbm, cache_hbm, group_hbm, up_key_hbm, up_value_hbm, w_hbm,
    out_ref,
    q_nope, q_rope, cache, group, up_key, up_value, w,
    kv, q, acc, m_ref, l_ref, h_out,
    sd, rd, sx, rx, racc, sy, ry, sf, rf,
    in_sem, z_send, z_recv, x_send, x_recv, d_send, d_recv,
    rd_send, rd_recv, rx_send, rx_recv, ry_send, ry_recv, rf_send, rf_recv,
):
    c = lax.axis_index("ctx")
    t = lax.axis_index("tp")
    z, xh = c // 2, c % 2
    xl, y, k = t // 16, (t // 2) % 8, t % 2
    dk = 1 - 2 * k
    half = 80 * k

    def dev(cc, tt):
        return (cc, tt)

    z_next = dev(((z + dk + NZ) % NZ) * 2 + xh, t)
    z_prev = dev(((z - dk + NZ) % NZ) * 2 + xh, t)
    cross = dev(z * 2 + 1 - xh, (1 - xl) * 16 + y * 2 + k)
    inner = dev(c, (1 - xl) * 16 + y * 2 + k)
    partner = dev(c, xl * 16 + y * 2 + 1 - k)

    def y_peer(o):
        return dev(c, xl * 16 + ((y + o) % NY) * 2 + k)

    loads = [
        pltpu.make_async_copy(src, dst, in_sem.at[i])
        for i, (src, dst) in enumerate(
            [(group_hbm, group), (cache_hbm, cache), (q_nope_hbm, q_nope), (up_key_hbm, up_key), (q_rope_hbm, q_rope),
             (up_value_hbm, up_value), (w_hbm, w)]
        )
    ]
    for load in loads:
        load.start()

    barrier = pltpu.get_barrier_semaphore()
    for peer in [z_next, z_prev, cross, inner, partner]:
        pl.semaphore_signal(barrier, inc=1, device_id=peer, device_id_type=MESH)
    for o in range(1, NY):
        pl.semaphore_signal(barrier, inc=1, device_id=y_peer(o), device_id_type=MESH)

    lane = lax.broadcasted_iota(jnp.int32, (TOK, 128), 1)
    row = lax.broadcasted_iota(jnp.int32, (TOK, 128), 0)
    angles = (offset_ref[0] + c * TOK + row).astype(F32) * freq_ref[...]
    cosine, sine = jnp.cos(angles), jnp.sin(angles)
    sine = jnp.where(lane % 64 < 32, -sine, sine)

    def rotate(v):
        other = jnp.where(lane % 64 < 32, pltpu.roll(v, 96, 1), pltpu.roll(v, 32, 1))
        return v * cosine + other * sine

    own = slot(0, 0, 0)
    loads[0].wait()
    loads[1].wait()
    kv[own : own + CACHED, 0:LATENT] = cache[:, 0:LATENT]
    zeros = jnp.zeros((CACHED, 64), BF16)
    kv[own : own + CACHED, LATENT:WIDE] = jnp.concatenate([cache[:, LATENT : LATENT + ROPE], zeros], 1)
    kv[own + CACHED : own + SPAN, 0:LATENT] = group[:, 0:LATENT]
    tail = group[:, LATENT : LATENT + ROPE].astype(F32)
    tail = rotate(jnp.concatenate([tail, tail], 1))
    kv[own + CACHED : own + SPAN, LATENT:WIDE] = jnp.where(lane < 64, tail, 0.0).astype(BF16)

    pl.semaphore_wait(barrier, 12)

    def send(src, dst, s_sem, r_sem, to):
        pltpu.make_async_remote_copy(src_ref=src, dst_ref=dst, send_sem=s_sem, recv_sem=r_sem, device_id=to, device_id_type=MESH).start()

    def arrival(view, r_sem):
        pltpu.make_async_remote_copy(src_ref=view, dst_ref=view, send_sem=r_sem, recv_sem=r_sem, device_id=partner, device_id_type=MESH).wait_recv()

    def sent(view, s_sem):
        pltpu.make_async_remote_copy(src_ref=view, dst_ref=view, send_sem=s_sem, recv_sem=s_sem, device_id=partner, device_id_type=MESH).wait_send()

    for j in range(5):
        send(rows_at(kv, slot(0, 0, 0) + 32 * j, 32), rows_at(kv, slot(1, 0, 0) + 32 * j, 32), z_send.at[0], z_recv.at[0, j], z_next)
    send(rows_at(kv, slot(0, 0, 0) + half, 80), rows_at(kv, slot(0, 0, 1) + half, 80), x_send.at[0], x_recv.at[0, 0], cross)

    loads[2].wait()
    loads[3].wait()
    loads[4].wait()
    for h in range(HEADS):
        lat = jnp.dot(q_nope[:, h * NOPE : (h + 1) * NOPE], up_key[h], preferred_element_type=F32)
        q[h * TOK : (h + 1) * TOK, 0:LATENT] = lat.astype(BF16)
    for pair in range(HEADS // 2):
        turned = rotate(q_rope[:, pair * 128 : (pair + 1) * 128].astype(F32))
        for part in range(2):
            moved = turned if part == 0 else pltpu.roll(turned, 64, 1)
            h = 2 * pair + part
            q[h * TOK : (h + 1) * TOK, LATENT:WIDE] = jnp.where(lane < 64, moved, 0.0).astype(BF16)
    m_ref[...] = jnp.full(m_ref.shape, NEG, F32)
    l_ref[...] = jnp.zeros(l_ref.shape, F32)
    acc[...] = jnp.zeros(acc.shape, F32)

    key_lane = lax.broadcasted_iota(jnp.int32, (1, CHUNK), 1)
    key_block = key_lane // SPAN
    key_slot = key_lane % SPAN

    def bias_of(owners):
        count = jnp.zeros((1, CHUNK), jnp.int32)
        earlier = jnp.zeros((1, CHUNK), jnp.int32)
        for b, owner in enumerate(owners):
            count = jnp.where(key_block == b, counts_ref[owner], count)
            earlier = jnp.where(key_block == b, jnp.where(owner < c, 1, 0), earlier)
        live = (key_slot < CACHED) & (key_slot < count)
        seen = live | ((key_slot >= CACHED) & (earlier > 0))
        return jnp.where(seen, 0.0, NEG).astype(F32)

    def fold(base, g, bias, own_rows):
        r0 = g * GROUP
        if not isinstance(base, int):
            base = pl.multiple_of(base, 128)
        keys = kv[pl.ds(base, CHUNK), :]
        s = lax.dot_general(q[r0 : r0 + GROUP, :], keys, (((1,), (1,)), ((), ())), preferred_element_type=F32)
        s = s * SCALE + bias
        if own_rows:
            token = lax.broadcasted_iota(jnp.int32, (GROUP, CHUNK), 0) % TOK
            key = lax.broadcasted_iota(jnp.int32, (GROUP, CHUNK), 1)
            hidden = (key >= CACHED) & (key < SPAN) & (key - CACHED > token)
            s = jnp.where(hidden, NEG, s)
        old = m_ref[r0 : r0 + GROUP, :]
        top = jnp.maximum(old, jnp.max(s, axis=1, keepdims=True))
        alpha = jnp.exp2(old - top)
        e = jnp.exp2(s - top[:, 0:1])
        m_ref[r0 : r0 + GROUP, :] = top
        l_ref[r0 : r0 + GROUP, :] = l_ref[r0 : r0 + GROUP, :] * alpha + jnp.sum(e, axis=1, keepdims=True)
        mixed = jnp.dot(e.astype(BF16), keys[:, 0:LATENT], preferred_element_type=F32)
        acc[r0 : r0 + GROUP, :] = acc[r0 : r0 + GROUP, :] * alpha[:, 0:1] + mixed

    def forwards(i):
        return (z + i + xl + k) % 2 == 0

    def piece(i, j):
        if isinstance(i, int) and i == 6:
            return half + 16 * j, 16
        return 32 * j, 32

    def whole(i):
        if isinstance(i, int) and i in (0, 6):
            return half, 80
        return 0, SPAN

    def x_out(i, j, o, to):
        r, size = piece(i, j)
        send(rows_at(kv, slot(i, 0, o) + r, size), rows_at(kv, slot(i, 0, 1) + r, size), x_send.at[i], x_recv.at[i, j], to)

    def d_out(i, o):
        r, size = whole(i)
        s = 0 if isinstance(i, int) and i in (0, 6) else 1
        send(rows_at(kv, slot(i, 0, o) + r, size), rows_at(kv, slot(i, s, o) + r, size), d_send.at[i, o], d_recv.at[i, o], partner)

    def d_in(i, o):
        if isinstance(i, int) and i in (0, 6):
            view = rows_at(kv, slot(i, 0, o) + 80 - half, 80)
        else:
            view = rows_at(kv, slot(i, 1, o), SPAN)
        arrival(view, d_recv.at[i, o])

    def guarded(test, fn):
        if isinstance(test, bool):
            if test:
                fn()
        else:
            pl.when(test)(fn)

    def step(n, compute):
        static = isinstance(n, int)
        z_on = (n <= 6) if static else True
        for j in range(5):
            if z_on:
                r, size = piece(n, j)
                arrival(rows_at(kv, slot(n, 0, 0) + r, size), z_recv.at[n - 1, j])
                if not static:
                    def on_z(j=j, r=r, size=size):
                        send(rows_at(kv, slot(n, 0, 0) + r, size), rows_at(kv, slot(n + 1, 0, 0) + r, size), z_send.at[n], z_recv.at[n, j], z_next)
                    guarded(n < 5, on_z)
                guarded(jnp.logical_not(forwards(n)), lambda j=j: x_out(n, j, 0, cross))
            m = n - 1
            if not static or m <= 6:
                def inner_out(j=j):
                    r, size = piece(m, j)
                    arrival(rows_at(kv, slot(m, 0, 1) + r, size), x_recv.at[m, j])
                    x_out(m, j, 1, inner)
                test = forwards(m)
                guarded(test if static else test & (m >= 1), inner_out)
            if compute is not None and j in (1, 3):
                compute(j // 2)
        if not static:
            @pl.when(n == 5)
            def _():
                for j in range(5):
                    r = half + 16 * j
                    send(rows_at(kv, slot(5, 0, 0) + r, 16), rows_at(kv, slot(6, 0, 0) + r, 16), z_send.at[5], z_recv.at[5, j], z_next)
        if z_on:
            d_out(n, 0)
        m = n - 1
        if not static or m <= 6:
            test = forwards(m)
            guarded(test if static else test & (m >= 1), lambda: d_out(m, 1))
        p = n - 2
        def late():
            for j in range(5):
                r, size = piece(p, j)
                arrival(rows_at(kv, slot(p, 0, 1) + r, size), x_recv.at[p, j])
            d_out(p, 1)
        test = jnp.logical_not(forwards(p))
        guarded(test if static else test & (p >= 1), late)

    def owners_of(i):
        near, far = (z - dk * i + NZ) % NZ, (z + dk * i + NZ) % NZ
        return [near * 2 + xh, near * 2 + 1 - xh, far * 2 + xh, far * 2 + 1 - xh]

    def fold_chunk(i):
        bias = bias_of(owners_of(i))
        def run(g):
            if g == 0:
                d_in(i, 0)
                d_in(i, 1)
            fold((i - 1) * CHUNK, g, bias, False)
        return run

    @pl.loop(1, 6)
    def _(n):
        def compute(g):
            @pl.when(n >= 4)
            def _():
                fold_chunk(n - 3)(g)
        step(n, compute)

        @pl.when(n == 2)
        def _():
            arrival(rows_at(kv, slot(0, 0, 1) + half, 80), x_recv.at[0, 0])
            d_out(0, 1)

    for n in (6, 7, 8):
        step(n, fold_chunk(n - 3))
    d_in(0, 1)
    d_in(6, 0)
    d_in(6, 1)
    far = (z + 6) % NZ
    bias = bias_of([c, z * 2 + 1 - xh, far * 2 + xh, far * 2 + 1 - xh])
    bias = jnp.where((key_lane >= CACHED) & (key_lane < SPAN), 0.0, bias)
    for g in range(ROWS // GROUP):
        fold(5 * CHUNK, g, bias, True)

    loads[5].wait()
    for h in range(HEADS):
        inverse = 1.0 / l_ref[h * TOK : (h + 1) * TOK, 0:1]
        attended = (acc[h * TOK : (h + 1) * TOK, :] * inverse).astype(BF16)
        h_out[:, h * VDIM : (h + 1) * VDIM] = jnp.dot(attended, up_value[h], preferred_element_type=F32).astype(BF16)
    loads[6].wait()

    def offset_of(i):
        return jnp.where(i % 2 == 1, 4 - (i + 1) // 2, 4 + i // 2) % NY

    def window(x_side, i):
        yy = (y + offset_of(i)) % NY
        start = x_side * 3584 + yy * 448 - 64 * (yy % 2)
        cols = w[:, pl.ds(pl.multiple_of(start, 128), WIN)]
        return jnp.dot(h_out[...], cols, preferred_element_type=F32)

    LAG = 2

    @pl.loop(0, NY + LAG)
    def _(n):
        @pl.when(n < NY)
        def _():
            sd[n] = window(1 - k, n).astype(BF16)
            send(sd.at[n], rd.at[n], rd_send.at[n], rd_recv.at[n], partner)

        @pl.when(n >= LAG)
        def _():
            i = n - LAG
            mine = window(k, i)
            arrival(rd.at[i], rd_recv.at[i])
            total = mine + rd[i].astype(F32)

            @pl.when(k == xl)
            def _():
                racc[i] = total

            @pl.when(k != xl)
            def _():
                sx[i] = total.astype(BF16)
                send(sx.at[i], rx.at[i], rx_send.at[i], rx_recv.at[i], inner)

    def take(total, kk):
        start = 64 * (y % 2) + 224 * kk
        return pltpu.roll(total, (WIN - start) % WIN, 1)[:, 0:256].astype(BF16)

    @pl.when(k == xl)
    def _():
        @pl.loop(0, NY - 1)
        def _(i):
            arrival(rx.at[i], rx_recv.at[i])
            sy[i] = (racc[i] + rx[i].astype(F32)).astype(BF16)
            send(sy.at[i], ry.at[i], ry_send.at[i], ry_recv.at[i], y_peer(offset_of(i)))

        arrival(rx.at[NY - 1], rx_recv.at[NY - 1])
        racc[NY - 1] = racc[NY - 1] + rx[NY - 1].astype(F32)

        @pl.loop(0, NY - 1)
        def _(i):
            arrival(ry.at[i], ry_recv.at[i])
            racc[NY - 1] = racc[NY - 1] + ry[i].astype(F32)

        total = racc[NY - 1]
        sf[...] = take(total, 1 - k)
        send(sf, rf, rf_send.at[0], rf_recv.at[0], partner)
        out_ref[...] = take(total, k)[:, 0:224]

    @pl.when(k != xl)
    def _():
        arrival(rf, rf_recv.at[0])
        out_ref[...] = rf[:, 0:224]

    for i in range(5):
        sent(rows_at(kv, 0, SPAN), z_send.at[i])
    sent(rows_at(kv, 0, 80), z_send.at[5])
    for i in range(7):
        sent(rows_at(kv, 0, whole(i)[1]), x_send.at[i])
        for o in range(2):
            if i or o:
                sent(rows_at(kv, 0, whole(i)[1]), d_send.at[i, o])

    @pl.loop(0, NY)
    def _(i):
        sent(sd.at[i], rd_send.at[i])

    @pl.when(k != xl)
    def _():
        @pl.loop(0, NY)
        def _(i):
            sent(sx.at[i], rx_send.at[i])

    @pl.when(k == xl)
    def _():
        @pl.loop(0, NY - 1)
        def _(i):
            sent(sy.at[i], ry_send.at[i])

        sent(sf, rf_send.at[0])


def local(q_nope, q_rope, cache_latent, group_latent, offset, counts, up_key, up_value, out_weight):
    k32 = np.arange(128) % 32
    freq = jnp.asarray((10000.0 ** (-2.0 * k32 / ROPE)).astype(np.float32)[None, :])
    any_spec = pl.BlockSpec(memory_space=pl.ANY)
    smem = pl.BlockSpec(memory_space=pltpu.SMEM)
    vmem = pl.BlockSpec(memory_space=pltpu.VMEM)
    dma = pltpu.SemaphoreType.DMA
    win = (TOK, WIN)
    return pl.pallas_call(
        kernel,
        out_shape=jax.ShapeDtypeStruct((TOK, 224), BF16),
        in_specs=[smem, smem, vmem] + [any_spec] * 7,
        out_specs=vmem,
        scratch_shapes=[
            pltpu.VMEM((TOK, HEADS * NOPE), BF16),
            pltpu.VMEM((TOK, HEADS * ROPE), BF16),
            pltpu.VMEM((CACHED, LATENT + ROPE), BF16),
            pltpu.VMEM((TOK, LATENT + ROPE), BF16),
            pltpu.VMEM((HEADS, NOPE, LATENT), BF16),
            pltpu.VMEM((HEADS, LATENT, VDIM), BF16),
            pltpu.VMEM((HEADS * VDIM, 7168), BF16),
            pltpu.VMEM((6 * CHUNK, WIDE), BF16),
            pltpu.VMEM((ROWS, WIDE), BF16),
            pltpu.VMEM((ROWS, LATENT), F32),
            pltpu.VMEM((ROWS, 128), F32),
            pltpu.VMEM((ROWS, 128), F32),
            pltpu.VMEM((TOK, HEADS * VDIM), BF16),
            pltpu.VMEM((NY, *win), BF16),
            pltpu.VMEM((NY, *win), BF16),
            pltpu.VMEM((NY, *win), BF16),
            pltpu.VMEM((NY, *win), BF16),
            pltpu.VMEM((NY, *win), F32),
            pltpu.VMEM((NY - 1, *win), BF16),
            pltpu.VMEM((NY - 1, *win), BF16),
            pltpu.VMEM((TOK, 256), BF16),
            pltpu.VMEM((TOK, 256), BF16),
            dma((7,)), dma((6,)), dma((6, 5)), dma((7,)), dma((7, 5)), dma((7, 2)), dma((7, 2)),
            dma((NY,)), dma((NY,)), dma((NY,)), dma((NY,)), dma((NY - 1,)), dma((NY - 1,)), dma((1,)), dma((1,)),
        ],
        compiler_params=pltpu.CompilerParams(collective_id=0, has_side_effects=True, vmem_limit_bytes=60000 * 1024),
    )(offset, counts, freq, q_nope, q_rope, cache_latent, group_latent, up_key, up_value, out_weight)


def solution(mesh):
    in_specs = (
        P("ctx", "tp"), P("ctx", "tp"), P("ctx", None), P("ctx", None), P(), P(),
        P("tp", None, None), P("tp", None, None), P("tp", None),
    )
    return jax.shard_map(local, mesh=mesh, in_specs=in_specs, out_specs=P("ctx", "tp"), check_vma=False)
```

```python
import math

import jax
import jax.numpy as jnp
import numpy as np
from jax import lax
from jax.experimental import pallas as pl
from jax.experimental.pallas import tpu as pltpu
from jax.sharding import PartitionSpec as P

LATENT = 512
ROPE = 64
NOPE = 128
VDIM = 128
WIDE = 640
NZ = 12
NY = 8
TOK = 128
CACHED = 32
HEADS = 4
ROWS = TOK * HEADS
UP = 6
DOWN = 5
OWN = 11
HALF = 64
CH = 16
WIN = 512
NEG = -1e30
SCALE = math.log2(math.e) / math.sqrt(NOPE + ROPE)
GROUP = 256
MESH = pl.DeviceIdType.MESH
F32 = jnp.float32
BF16 = jnp.bfloat16


def group_row(slot, o):
    return slot * 256 + o * TOK


def cache_row(half, o, zs):
    return ((half * 2 + o) * NZ + zs) * CH


def rows_at(ref, start, size):
    if not isinstance(start, int):
        start = pl.multiple_of(start, 16)
    return ref.at[pl.ds(start, size), :]


def kernel(
    offset_hbm, counts_hbm, freq_hbm, q_nope_hbm, q_rope_hbm, cache_hbm, group_hbm, up_key_hbm, up_value_hbm, w_hbm,
    out_ref,
    offset_ref, counts_ref, freq_ref, q_nope, q_rope, cache, group, up_key, up_value, w,
    kg, kc, q, acc, m_ref, l_ref, h_out,
    sd, rd, sx, rx, racc, sy, ry, sf, rf, total_t,
    in_sem, gz_send, gz_recv, gx_send, gx_recv, gd_send, gd_recv, cz_send, cz_recv, cx_send, cx_recv, cd_send, cd_recv,
    rd_send, rd_recv, rx_send, rx_recv, ry_send, ry_recv, rf_send, rf_recv,
):
    c = lax.axis_index("ctx")
    t = lax.axis_index("tp")
    z, xh = c // 2, c % 2
    xl, y, k = t // 16, (t // 2) % 8, t % 2

    def dev(cc, tt):
        return (cc, tt)

    above = dev(((z + 1) % NZ) * 2 + xh, t)
    below = dev(((z + NZ - 1) % NZ) * 2 + xh, t)
    cross = dev(z * 2 + 1 - xh, (1 - xl) * 16 + y * 2 + k)
    inner = dev(c, (1 - xl) * 16 + y * 2 + k)
    partner = dev(c, xl * 16 + y * 2 + 1 - k)

    def y_peer(o):
        return dev(c, xl * 16 + ((y + o) % NY) * 2 + k)

    loads = [
        pltpu.make_async_copy(src, dst, in_sem.at[i])
        for i, (src, dst) in enumerate(
            [(group_hbm, group), (cache_hbm, cache), (offset_hbm, offset_ref), (counts_hbm, counts_ref), (freq_hbm, freq_ref), (q_nope_hbm, q_nope), (up_key_hbm, up_key), (q_rope_hbm, q_rope),
             (up_value_hbm, up_value), (w_hbm, w)]
        )
    ]
    for load in loads:
        load.start()

    barrier = pltpu.get_barrier_semaphore()
    for peer in [below, above, cross, inner, partner, y_peer(1), y_peer(NY - 1)]:
        pl.semaphore_signal(barrier, inc=1, device_id=peer, device_id_type=MESH)

    @pl.loop(jnp.maximum(DOWN, z + 2), jnp.where(z == 0, NZ - 1, NZ))
    def _(zh):
        pl.semaphore_signal(barrier, inc=1, device_id=dev(zh * 2 + xh, t), device_id_type=MESH)

    for i in (2, 3, 4):
        loads[i].wait()

    lane = lax.broadcasted_iota(jnp.int32, (TOK, 128), 1)
    row = lax.broadcasted_iota(jnp.int32, (TOK, 128), 0)
    angles = (offset_ref[0] + c * TOK + row).astype(F32) * freq_ref[...]
    cosine, sine = jnp.cos(angles), jnp.sin(angles)
    sine = jnp.where(lane % 64 < 32, -sine, sine)

    def rotate(v):
        other = jnp.where(lane % 64 < 32, pltpu.roll(v, 96, 1), pltpu.roll(v, 32, 1))
        return v * cosine + other * sine

    own = group_row(OWN, 0)
    loads[0].wait()
    loads[1].wait()
    lane16 = lane[0:CH]
    rows, into = pl.ds(pl.multiple_of(CH * k, CH), CH), pl.ds(pl.multiple_of(cache_row(k, 0, z), CH), CH)
    dead = jnp.where((lane16 == 64) & (row[0:CH] + CH * k >= counts_ref[c]), 1.0, 0.0)
    held = cache[rows, LATENT : LATENT + ROPE].astype(F32)
    held = jnp.concatenate([held, held], 1)
    kc[into, 0:LATENT] = cache[rows, 0:LATENT]
    kc[into, LATENT:WIDE] = jnp.where(lane16 < 64, held, dead).astype(BF16)
    for part in range(LATENT // 128):
        cols = slice(part * 128, (part + 1) * 128)
        kg[own : own + TOK, cols] = group[cols, :].T
    tail = group[LATENT : LATENT + ROPE, :].astype(F32)
    tail = rotate(jnp.concatenate([tail, tail], 0).T)
    owned = jnp.where(lane == 65 + c, 1.0, 0.0)
    kg[own : own + TOK, LATENT:WIDE] = jnp.where(lane < 64, tail, owned).astype(BF16)

    pl.semaphore_wait(barrier, 7 + jnp.where(z >= DOWN, z - 1 - z // (NZ - 1), 0))

    def send(src, dst, s_sem, r_sem, to):
        pltpu.make_async_remote_copy(src_ref=src, dst_ref=dst, send_sem=s_sem, recv_sem=r_sem, device_id=to, device_id_type=MESH).start()

    def arrival(view, r_sem):
        pltpu.make_async_remote_copy(src_ref=view, dst_ref=view, send_sem=r_sem, recv_sem=r_sem, device_id=partner, device_id_type=MESH).wait_recv()

    def sent(view, s_sem):
        pltpu.make_async_remote_copy(src_ref=view, dst_ref=view, send_sem=s_sem, recv_sem=s_sem, device_id=partner, device_id_type=MESH).wait_send()

    mine = HALF * k

    def group_half(slot, o, r=0, size=HALF):
        return rows_at(kg, group_row(slot, o) + mine + r, size)

    def cache_half(o, zs, size=CH):
        return rows_at(kc, cache_row(k, o, zs), size)

    def first_send(slot, s_sem, to):
        for j in range(4):
            send(group_half(OWN, 0, CH * j, CH), group_half(slot, 0, CH * j, CH), s_sem, gz_recv.at[slot, j], to)
        send(cache_half(0, z), cache_half(0, z), s_sem, gz_recv.at[slot, 4], to)

    pl.when(z < NZ - 1)(lambda: first_send(0, gz_send.at[11], above))
    pl.when(z < DOWN)(lambda: first_send(10, gz_send.at[12], below))

    @pl.when(z >= DOWN)
    def _():
        @pl.loop(0, z)
        def _(zl):
            send(cache_half(0, z), cache_half(0, z), cz_send.at[zl], cz_recv.at[z], dev(zl * 2 + xh, t))

    send(cache_half(0, z), cache_half(1, z), cx_send.at[z], cx_recv.at[z], cross)
    send(group_half(OWN, 0), group_half(OWN, 1), gx_send.at[OWN], gx_recv.at[OWN, 0], cross)

    loads[5].wait()
    loads[6].wait()
    loads[7].wait()
    for h in range(HEADS):
        lat = jnp.dot(q_nope[:, h * NOPE : (h + 1) * NOPE], up_key[h], preferred_element_type=F32)
        q[h * TOK : (h + 1) * TOK, 0:LATENT] = (lat * SCALE).astype(BF16)
    hides = jnp.where((lane == 64) | ((lane > 65 + c) & (lane < 65 + 24)), NEG, 0.0)
    for pair in range(HEADS // 2):
        turned = rotate(q_rope[:, pair * 128 : (pair + 1) * 128].astype(F32)) * SCALE
        for part in range(2):
            moved = turned if part == 0 else pltpu.roll(turned, 64, 1)
            h = 2 * pair + part
            q[h * TOK : (h + 1) * TOK, LATENT:WIDE] = jnp.where(lane < 64, moved, hides).astype(BF16)
    m_ref[...] = jnp.full(m_ref.shape, NEG, F32)
    l_ref[...] = jnp.zeros(l_ref.shape, F32)
    acc[...] = jnp.zeros(acc.shape, F32)

    def fold(ref, base, size, last=False):
        for g in range(ROWS // GROUP):
            r = slice(g * GROUP, (g + 1) * GROUP)
            keys = rows_at(ref, base, size)[...]
            s = lax.dot_general(q[r, :], keys, (((1,), (1,)), ((), ())), preferred_element_type=F32)
            if last:
                token = lax.broadcasted_iota(jnp.int32, (GROUP, TOK), 0) % TOK
                key = lax.broadcasted_iota(jnp.int32, (GROUP, TOK), 1)
                masked = jnp.where(key > token, NEG, s[:, size - 256 : size - TOK])
                s = jnp.concatenate([s[:, 0 : size - 256], masked, s[:, size - TOK :]], 1) if size > 256 else jnp.concatenate([masked, s[:, TOK:]], 1)
            old = m_ref[r, 0:1]
            top = jnp.maximum(old, jnp.max(s, axis=1, keepdims=True))
            alpha = jnp.exp2(old - top)
            e = jnp.exp2(s - top)
            total = jnp.sum(e, axis=1, keepdims=True) + l_ref[r, 0:1] * alpha
            mixed = jnp.dot(e.astype(BF16), keys[:, 0:LATENT], preferred_element_type=F32) + acc[r, :] * alpha
            m_ref[r, :] = jnp.broadcast_to(top, (GROUP, 128))
            l_ref[r, :] = jnp.broadcast_to(total, (GROUP, 128))
            acc[r, :] = mixed

    def forwards(i):
        return (z + i + xl + k) % 2 == 0

    def x_out(slot, j, o, to):
        send(group_half(slot, o, CH * j, CH), group_half(slot, 1, CH * j, CH), gx_send.at[slot], gx_recv.at[slot, j], to)

    def d_out(slot, o):
        send(group_half(slot, o), group_half(slot, o), gd_send.at[slot, o], gd_recv.at[slot, o], partner)

    def d_in(slot, o):
        arrival(rows_at(kg, group_row(slot, o) + HALF - mine, HALF), gd_recv.at[slot, o])

    def block_piece(n, j, slot, has, needed, onward, to, step):
        @pl.when(has)
        def _():
            arrival(group_half(slot, 0, CH * j, CH), gz_recv.at[slot, j])

            @pl.when(onward)
            def _():
                send(group_half(slot, 0, CH * j, CH), group_half(slot + step, 0, CH * j, CH), gz_send.at[slot], gz_recv.at[slot + step, j], to)

            @pl.when(needed & jnp.logical_not(forwards(n)))
            def _():
                x_out(slot, j, 0, cross)

    def inner_step(n, slot):
        @pl.when(forwards(n))
        def _():
            for j in range(4):
                arrival(group_half(slot, 1, CH * j, CH), gx_recv.at[slot, j])
                x_out(slot, j, 1, inner)
            d_out(slot, 1)

    def late_step(n, slot):
        @pl.when(jnp.logical_not(forwards(n)))
        def _():
            for j in range(4):
                arrival(group_half(slot, 1, CH * j, CH), gx_recv.at[slot, j])
            d_out(slot, 1)

    def ring_cache(slot, zs, has, onward, to, step):
        @pl.when(has)
        def _():
            arrival(cache_half(0, zs), gz_recv.at[slot, 4])

            @pl.when(onward)
            def _():
                send(cache_half(0, zs), cache_half(0, zs), gz_send.at[slot], gz_recv.at[slot + step, 4], to)

            cache_cross(zs)

    def cache_cross(zs):
        @pl.when((zs + xl) % 2 == 1)
        def _():
            send(cache_half(0, zs), cache_half(1, zs), cx_send.at[zs], cx_recv.at[zs], cross)

    def cache_inner(zs):
        @pl.when((zs + xl) % 2 == 0)
        def _():
            arrival(cache_half(1, zs), cx_recv.at[zs])
            send(cache_half(1, zs), cache_half(1, zs), cx_send.at[zs], cx_recv.at[zs], inner)

    def has_up(n):
        return (n >= 1) & (n <= UP) & (z >= n)

    def has_down(n):
        return (n >= 1) & (n <= DOWN) & ((z + n) % NZ < DOWN)

    def straight(n, i):
        zs = jnp.maximum(DOWN, z + 1) + 2 * (n - 1) + i
        return zs, (n >= 1) & (zs < NZ)

    def up_needed(i):
        return (i >= 1) & (i <= UP) & (z >= i)

    def down_needed(i):
        return (i >= 1) & (i <= DOWN) & (z + i >= NZ)

    def fold_slots(first):
        for i in range(4):
            @pl.when(z > first + i)
            def _(i=i):
                d_in(first + i, 0)
                d_in(first + i, 1)

        @pl.when(z >= first + 4)
        def _():
            fold(kg, first * 256, 1024)

        @pl.when((z > first) & (z < first + 4))
        def _():
            @pl.when(z > first + 1)
            def _():
                fold(kg, first * 256, 512)

            @pl.when((z - first) % 2 == 1)
            def _():
                fold(kg, (first + (z - first) // 2 * 2) * 256, 256)

    @pl.loop(1, UP + 3)
    def _(n):
        for j in range(4):
            block_piece(n, j, n - 1, has_up(n), True, (n < UP) & (z < NZ - 1), above, 1)
            block_piece(n, j, 11 - n, has_down(n), z + n >= NZ, n < DOWN, below, -1)
        ring_cache(n - 1, z - n, has_up(n), (n < UP) & (z < NZ - 1), above, 1)
        ring_cache(11 - n, (z + n) % NZ, has_down(n), n < DOWN, below, -1)
        for i in range(2):
            zs, there = straight(n, i)

            @pl.when(there)
            def _(zs=zs):
                arrival(cache_half(0, zs), cz_recv.at[zs])
                cache_cross(zs)

        pl.when(up_needed(n))(lambda: d_out(n - 1, 0))
        pl.when(down_needed(n))(lambda: d_out(11 - n, 0))
        m, p = n - 1, n - 2
        pl.when(has_up(m))(lambda: cache_inner(z - m))
        pl.when(has_down(m))(lambda: cache_inner((z + m) % NZ))
        for i in range(2):
            zs, there = straight(m, i)
            pl.when(there)(lambda zs=zs: cache_inner(zs))
        pl.when(up_needed(m))(lambda: inner_step(m, m - 1))
        pl.when(down_needed(m))(lambda: inner_step(m, 11 - m))
        pl.when(up_needed(p))(lambda: late_step(p, p - 1))
        pl.when(down_needed(p))(lambda: late_step(p, 11 - p))

        @pl.when(n == 2)
        def _():
            arrival(group_half(OWN, 1), gx_recv.at[OWN, 0])
            d_out(OWN, 1)

        @pl.when(n == UP)
        def _():
            send(cache_half(0, 0, NZ * CH), cache_half(0, 0, NZ * CH), cd_send.at[0], cd_recv.at[0], partner)

        @pl.when(n == UP + 1)
        def _():
            fold_slots(0)

    @pl.loop(0, NZ)
    def _(zs):
        @pl.when(((zs + xl) % 2 == 1) | (zs == z))
        def _():
            arrival(cache_half(1, zs), cx_recv.at[zs])

    send(cache_half(1, 0, NZ * CH), cache_half(1, 0, NZ * CH), cd_send.at[1], cd_recv.at[1], partner)
    fold_slots(4)

    for o in range(2):
        arrival(rows_at(kc, cache_row(1 - k, o, 0), NZ * CH), cd_recv.at[o])
    fold(kc, 0, 2 * NZ * CACHED)

    @pl.when(z > 8)
    def _():
        d_in(8, 0)
        d_in(8, 1)

    @pl.when(z > 9)
    def _():
        d_in(9, 0)
        d_in(9, 1)
        fold(kg, 8 * 256, 512)

    @pl.when(z == 9)
    def _():
        fold(kg, 8 * 256, 256)

    d_in(OWN, 1)

    @pl.when(z == NZ - 1)
    def _():
        d_in(10, 0)
        d_in(10, 1)
        fold(kg, 10 * 256, 512, True)

    @pl.when(z < NZ - 1)
    def _():
        fold(kg, OWN * 256, 256, True)

    loads[8].wait()
    for h in range(HEADS):
        inverse = 1.0 / l_ref[h * TOK : (h + 1) * TOK, 0:1]
        attended = (acc[h * TOK : (h + 1) * TOK, :] * inverse).astype(BF16)
        h_out[:, h * VDIM : (h + 1) * VDIM] = jnp.dot(attended, up_value[h], preferred_element_type=F32).astype(BF16)
    loads[9].wait()

    def offset_of(i):
        return jnp.where(i % 2 == 1, 4 - (i + 1) // 2, 4 + i // 2) % NY

    def window(x_side, i):
        yy = (y + offset_of(i)) % NY
        start = x_side * 3584 + yy * 448 - 64 * (yy % 2)
        cols = w[:, pl.ds(pl.multiple_of(start, 128), WIN)]
        return jnp.dot(h_out[...], cols, preferred_element_type=F32)

    LAG = 2

    def part(ref, i, b):
        return ref.at[i, pl.ds(b * HALF, HALF), :]

    @pl.loop(0, NY + LAG)
    def _(n):
        @pl.when(n < NY)
        def _():
            sd[n] = window(1 - k, n).astype(BF16)
            send(sd.at[n], rd.at[n], rd_send.at[n], rd_recv.at[n], partner)

        @pl.when(n >= LAG)
        def _():
            i = n - LAG
            mine = window(k, i)
            arrival(rd.at[i], rd_recv.at[i])
            total = mine + rd[i].astype(F32)

            @pl.when(k == xl)
            def _():
                racc[i] = total

            @pl.when(k != xl)
            def _():
                sx[i] = total.astype(BF16)
                for b in range(2):
                    send(part(sx, i, b), part(rx, i, b), rx_send.at[i], rx_recv.at[i, b], inner)

    @pl.when(k == xl)
    def _():
        @pl.loop(0, NY - 1)
        def _(i):
            for b in range(2):
                rows = slice(b * HALF, (b + 1) * HALF)
                arrival(part(rx, i, b), rx_recv.at[i, b])
                racc[i, rows, :] = racc[i, rows, :] + rx[i, rows, :].astype(F32)

                @pl.when(i >= 2)
                def _():
                    arrival(part(ry, i - 2, b), ry_recv.at[i - 2, b])
                    racc[i, rows, :] = racc[i, rows, :] + ry[i - 2, rows, :].astype(F32)

                sy[i, rows, :] = racc[i, rows, :].astype(BF16)
                send(part(sy, i, b), part(ry, i, b), ry_send.at[i], ry_recv.at[i, b], y_peer(NY - 1 - (i % 2) * (NY - 2)))

        for b in range(2):
            arrival(part(rx, NY - 1, b), rx_recv.at[NY - 1, b])
        racc[NY - 1] = racc[NY - 1] + rx[NY - 1].astype(F32)
        for i in (NY - 3, NY - 2):
            for b in range(2):
                arrival(part(ry, i, b), ry_recv.at[i, b])
            racc[NY - 1] = racc[NY - 1] + ry[i].astype(F32)
        total_t[...] = racc[NY - 1].T
        sf[...] = total_t[pl.ds(pl.multiple_of(64 * (y % 2) + 224 * (1 - k), 32), 224), :].astype(BF16)
        send(sf, rf, rf_send.at[0], rf_recv.at[0], partner)
        out_ref[...] = total_t[pl.ds(pl.multiple_of(64 * (y % 2) + 224 * k, 32), 224), :].astype(BF16)

    @pl.when(k != xl)
    def _():
        arrival(rf, rf_recv.at[0])
        out_ref[...] = rf[...]

    half_rows = rows_at(kg, 0, HALF)
    block_rows = rows_at(kg, 0, HALF + CH)
    pl.when(z < NZ - 1)(lambda: sent(block_rows, gz_send.at[11]))
    pl.when(z < DOWN)(lambda: sent(block_rows, gz_send.at[12]))
    sent(half_rows, gx_send.at[OWN])
    sent(half_rows, gd_send.at[OWN, 1])

    @pl.loop(1, UP + 1)
    def _(n):
        pl.when((n < UP) & (z < NZ - 1) & has_up(n))(lambda: sent(block_rows, gz_send.at[n - 1]))
        pl.when((n < DOWN) & has_down(n))(lambda: sent(block_rows, gz_send.at[11 - n]))

    @pl.loop(0, z)
    def _(i):
        sent(half_rows, gx_send.at[i])
        sent(half_rows, gd_send.at[i, 0])
        sent(half_rows, gd_send.at[i, 1])

    @pl.loop(0, NZ)
    def _(i):
        sent(rows_at(kc, 0, CH), cx_send.at[i])
        pl.when((z >= DOWN) & (i < z))(lambda: sent(rows_at(kc, 0, CH), cz_send.at[i]))

    for o in range(2):
        sent(rows_at(kc, 0, NZ * CH), cd_send.at[o])

    @pl.loop(0, NY)
    def _(i):
        sent(sd.at[i], rd_send.at[i])

    @pl.when(k != xl)
    def _():
        @pl.loop(0, NY)
        def _(i):
            sent(sx.at[i], rx_send.at[i])

    @pl.when(k == xl)
    def _():
        @pl.loop(0, NY - 1)
        def _(i):
            sent(sy.at[i], ry_send.at[i])

        sent(sf, rf_send.at[0])


def local(q_nope, q_rope, cache_latent, group_latent, offset, counts, up_key, up_value, out_weight):
    k32 = np.arange(128) % 32
    freq = jnp.asarray((10000.0 ** (-2.0 * k32 / ROPE)).astype(np.float32)[None, :])
    any_spec = pl.BlockSpec(memory_space=pl.ANY)
    vmem = pl.BlockSpec(memory_space=pltpu.VMEM)
    dma = pltpu.SemaphoreType.DMA
    win = (TOK, WIN)
    return pl.pallas_call(
        kernel,
        out_shape=jax.ShapeDtypeStruct((224, TOK), BF16),
        in_specs=[any_spec] * 10,
        out_specs=vmem,
        scratch_shapes=[
            pltpu.SMEM((1,), jnp.int32),
            pltpu.SMEM((24,), jnp.int32),
            pltpu.VMEM((1, 128), F32),
            pltpu.VMEM((TOK, HEADS * NOPE), BF16),
            pltpu.VMEM((TOK, HEADS * ROPE), BF16),
            pltpu.VMEM((CACHED, LATENT + ROPE), BF16),
            pltpu.VMEM((LATENT + ROPE, TOK), BF16),
            pltpu.VMEM((HEADS, NOPE, LATENT), BF16),
            pltpu.VMEM((HEADS, LATENT, VDIM), BF16),
            pltpu.VMEM((HEADS * VDIM, 7168), BF16),
            pltpu.VMEM((12 * 256, WIDE), BF16),
            pltpu.VMEM((2 * NZ * CACHED, WIDE), BF16),
            pltpu.VMEM((ROWS, WIDE), BF16),
            pltpu.VMEM((ROWS, LATENT), F32),
            pltpu.VMEM((ROWS, 128), F32),
            pltpu.VMEM((ROWS, 128), F32),
            pltpu.VMEM((TOK, HEADS * VDIM), BF16),
            pltpu.VMEM((NY, *win), BF16),
            pltpu.VMEM((NY, *win), BF16),
            pltpu.VMEM((NY, *win), BF16),
            pltpu.VMEM((NY, *win), BF16),
            pltpu.VMEM((NY, *win), F32),
            pltpu.VMEM((NY - 1, *win), BF16),
            pltpu.VMEM((NY - 1, *win), BF16),
            pltpu.VMEM((224, TOK), BF16),
            pltpu.VMEM((224, TOK), BF16),
            pltpu.VMEM((WIN, TOK), F32),
            dma((10,)), dma((13,)), dma((11, 5)), dma((12,)), dma((12, 4)), dma((12, 2)), dma((12, 2)),
            dma((12,)), dma((12,)), dma((12,)), dma((12,)), dma((2,)), dma((2,)),
            dma((NY,)), dma((NY,)), dma((NY,)), dma((NY, 2)), dma((NY - 1,)), dma((NY - 1, 2)), dma((1,)), dma((1,)),
        ],
        compiler_params=pltpu.CompilerParams(collective_id=0, has_side_effects=True, vmem_limit_bytes=60000 * 1024),
    )(offset, counts, freq, q_nope, q_rope, cache_latent, group_latent.T, up_key, up_value, out_weight).T


def solution(mesh):
    in_specs = (
        P("ctx", "tp"), P("ctx", "tp"), P("ctx", None), P("ctx", None), P(), P(),
        P("tp", None, None), P("tp", None, None), P("tp", None),
    )
    return jax.shard_map(local, mesh=mesh, in_specs=in_specs, out_specs=P("ctx", "tp"), check_vma=False)
```

```python
import math

import jax
import jax.numpy as jnp
import numpy as np
from jax import lax
from jax.experimental import pallas as pl
from jax.experimental.pallas import tpu as pltpu
from jax.sharding import PartitionSpec as P

LATENT = 512
ROPE = 64
NOPE = 128
VDIM = 128
WIDE = 640
NZ = 12
NY = 8
TOK = 128
CACHED = 32
HEADS = 4
ROWS = TOK * HEADS
UP = 6
DOWN = 5
OWN = 11
HALF = 64
CH = 16
WIN = 512
NEG = -1e30
SCALE = math.log2(math.e) / math.sqrt(NOPE + ROPE)
GROUP = 256
MESH = pl.DeviceIdType.MESH
F32 = jnp.float32
BF16 = jnp.bfloat16


def group_row(slot, o):
    return slot * 256 + o * TOK


def cache_row(half, o, zs):
    return ((half * 2 + o) * NZ + zs) * CH


def rows_at(ref, start, size):
    if not isinstance(start, int):
        start = pl.multiple_of(start, 16)
    return ref.at[pl.ds(start, size), :]


def kernel(
    offset_hbm, counts_hbm, freq_hbm, q_nope_hbm, q_rope_hbm, cache_hbm, group_hbm, up_key_hbm, up_value_hbm, w_hbm,
    out_ref,
    offset_ref, counts_ref, freq_ref, q_nope, q_rope, cache, group, up_key, up_value, w,
    kg, kc, q, acc, m_ref, l_ref, h_out,
    sd, rd, sx, rx, racc, sy, ry, sf, rf, total_t,
    in_sem, gz_send, gz_recv, gx_send, gx_recv, gd_send, gd_recv, cz_send, cz_recv, cx_send, cx_recv, cd_send, cd_recv,
    rd_send, rd_recv, rx_send, rx_recv, ry_send, ry_recv, rf_send, rf_recv,
):
    c = lax.axis_index("ctx")
    t = lax.axis_index("tp")
    z, xh = c // 2, c % 2
    xl, y, k = t // 16, (t // 2) % 8, t % 2

    def dev(cc, tt):
        return (cc, tt)

    above = dev(((z + 1) % NZ) * 2 + xh, t)
    below = dev(((z + NZ - 1) % NZ) * 2 + xh, t)
    cross = dev(z * 2 + 1 - xh, (1 - xl) * 16 + y * 2 + k)
    inner = dev(c, (1 - xl) * 16 + y * 2 + k)
    partner = dev(c, xl * 16 + y * 2 + 1 - k)

    def y_peer(o):
        return dev(c, xl * 16 + ((y + o) % NY) * 2 + k)

    loads = [
        pltpu.make_async_copy(src, dst, in_sem.at[i])
        for i, (src, dst) in enumerate(
            [(group_hbm, group), (cache_hbm, cache), (offset_hbm, offset_ref), (counts_hbm, counts_ref), (freq_hbm, freq_ref), (q_nope_hbm, q_nope), (up_key_hbm, up_key), (q_rope_hbm, q_rope),
             (up_value_hbm, up_value), (w_hbm, w)]
        )
    ]
    for load in loads:
        load.start()

    barrier = pltpu.get_barrier_semaphore()
    for peer in [below, above, cross, inner, partner, y_peer(1), y_peer(NY - 1)]:
        pl.semaphore_signal(barrier, inc=1, device_id=peer, device_id_type=MESH)

    @pl.loop(jnp.maximum(DOWN, z + 2), jnp.where(z == 0, NZ - 1, NZ))
    def _(zh):
        pl.semaphore_signal(barrier, inc=1, device_id=dev(zh * 2 + xh, t), device_id_type=MESH)

    for i in (2, 3, 4):
        loads[i].wait()

    lane = lax.broadcasted_iota(jnp.int32, (TOK, 128), 1)
    row = lax.broadcasted_iota(jnp.int32, (TOK, 128), 0)
    angles = (offset_ref[0] + c * TOK + row).astype(F32) * freq_ref[...]
    cosine, sine = jnp.cos(angles), jnp.sin(angles)
    sine = jnp.where(lane % 64 < 32, -sine, sine)

    def rotate(v):
        other = jnp.where(lane % 64 < 32, pltpu.roll(v, 96, 1), pltpu.roll(v, 32, 1))
        return v * cosine + other * sine

    own = group_row(OWN, 0)
    loads[0].wait()
    loads[1].wait()
    lane16 = lane[0:CH]
    rows, into = pl.ds(pl.multiple_of(CH * k, CH), CH), pl.ds(pl.multiple_of(cache_row(k, 0, z), CH), CH)
    dead = jnp.where((lane16 == 64) & (row[0:CH] + CH * k >= counts_ref[c]), 1.0, 0.0)
    held = cache[rows, LATENT : LATENT + ROPE].astype(F32)
    held = jnp.concatenate([held, held], 1)
    kc[into, 0:LATENT] = cache[rows, 0:LATENT]
    kc[into, LATENT:WIDE] = jnp.where(lane16 < 64, held, dead).astype(BF16)
    for part in range(LATENT // 128):
        cols = slice(part * 128, (part + 1) * 128)
        kg[own : own + TOK, cols] = group[cols, :].T
    tail = group[LATENT : LATENT + ROPE, :].astype(F32)
    tail = rotate(jnp.concatenate([tail, tail], 0).T)
    owned = jnp.where(lane == 65 + c, 1.0, 0.0)
    kg[own : own + TOK, LATENT:WIDE] = jnp.where(lane < 64, tail, owned).astype(BF16)

    pl.semaphore_wait(barrier, 7 + jnp.where(z >= DOWN, z - 1 - z // (NZ - 1), 0))

    def send(src, dst, s_sem, r_sem, to):
        pltpu.make_async_remote_copy(src_ref=src, dst_ref=dst, send_sem=s_sem, recv_sem=r_sem, device_id=to, device_id_type=MESH).start()

    def arrival(view, r_sem):
        pltpu.make_async_remote_copy(src_ref=view, dst_ref=view, send_sem=r_sem, recv_sem=r_sem, device_id=partner, device_id_type=MESH).wait_recv()

    def sent(view, s_sem):
        pltpu.make_async_remote_copy(src_ref=view, dst_ref=view, send_sem=s_sem, recv_sem=s_sem, device_id=partner, device_id_type=MESH).wait_send()

    mine = HALF * k

    def group_half(slot, o, r=0, size=HALF):
        return rows_at(kg, group_row(slot, o) + mine + r, size)

    def cache_half(o, zs, size=CH):
        return rows_at(kc, cache_row(k, o, zs), size)

    def first_send(slot, s_sem, to):
        for j in range(4):
            send(group_half(OWN, 0, CH * j, CH), group_half(slot, 0, CH * j, CH), s_sem, gz_recv.at[slot, j], to)
        send(cache_half(0, z), cache_half(0, z), s_sem, gz_recv.at[slot, 4], to)

    pl.when(z < NZ - 1)(lambda: first_send(0, gz_send.at[11], above))
    pl.when(z < DOWN)(lambda: first_send(10, gz_send.at[12], below))

    @pl.when(z >= DOWN)
    def _():
        @pl.loop(0, z)
        def _(zl):
            send(cache_half(0, z), cache_half(0, z), cz_send.at[zl], cz_recv.at[z], dev(zl * 2 + xh, t))

    send(cache_half(0, z), cache_half(1, z), cx_send.at[z], cx_recv.at[z], cross)
    send(group_half(OWN, 0), group_half(OWN, 1), gx_send.at[OWN], gx_recv.at[OWN, 0], cross)

    loads[5].wait()
    loads[6].wait()
    loads[7].wait()
    for h in range(HEADS):
        lat = jnp.dot(q_nope[:, h * NOPE : (h + 1) * NOPE], up_key[h], preferred_element_type=F32)
        q[h * TOK : (h + 1) * TOK, 0:LATENT] = (lat * SCALE).astype(BF16)
    hides = jnp.where((lane == 64) | ((lane > 65 + c) & (lane < 65 + 24)), NEG, 0.0)
    for pair in range(HEADS // 2):
        turned = rotate(q_rope[:, pair * 128 : (pair + 1) * 128].astype(F32)) * SCALE
        for part in range(2):
            moved = turned if part == 0 else pltpu.roll(turned, 64, 1)
            h = 2 * pair + part
            q[h * TOK : (h + 1) * TOK, LATENT:WIDE] = jnp.where(lane < 64, moved, hides).astype(BF16)
    m_ref[...] = jnp.full(m_ref.shape, NEG, F32)
    l_ref[...] = jnp.zeros(l_ref.shape, F32)
    acc[...] = jnp.zeros(acc.shape, F32)

    def fold(ref, base, size, last=False):
        for g in range(ROWS // GROUP):
            r = slice(g * GROUP, (g + 1) * GROUP)
            keys = rows_at(ref, base, size)[...]
            s = lax.dot_general(q[r, :], keys, (((1,), (1,)), ((), ())), preferred_element_type=F32)
            if last:
                token = lax.broadcasted_iota(jnp.int32, (GROUP, TOK), 0) % TOK
                key = lax.broadcasted_iota(jnp.int32, (GROUP, TOK), 1)
                masked = jnp.where(key > token, NEG, s[:, size - 256 : size - TOK])
                s = jnp.concatenate([s[:, 0 : size - 256], masked, s[:, size - TOK :]], 1) if size > 256 else jnp.concatenate([masked, s[:, TOK:]], 1)
            old = m_ref[r, 0:1]
            top = jnp.maximum(old, jnp.max(s, axis=1, keepdims=True))
            alpha = jnp.exp2(old - top)
            e = jnp.exp2(s - top)
            total = jnp.sum(e, axis=1, keepdims=True) + l_ref[r, 0:1] * alpha
            mixed = jnp.dot(e.astype(BF16), keys[:, 0:LATENT], preferred_element_type=F32) + acc[r, :] * alpha
            m_ref[r, :] = jnp.broadcast_to(top, (GROUP, 128))
            l_ref[r, :] = jnp.broadcast_to(total, (GROUP, 128))
            acc[r, :] = mixed

    def forwards(i):
        return (z + i + xl + k) % 2 == 0

    def x_out(slot, j, o, to):
        send(group_half(slot, o, CH * j, CH), group_half(slot, 1, CH * j, CH), gx_send.at[slot], gx_recv.at[slot, j], to)

    def d_out(slot, o):
        send(group_half(slot, o), group_half(slot, o), gd_send.at[slot, o], gd_recv.at[slot, o], partner)

    def d_in(slot, o):
        arrival(rows_at(kg, group_row(slot, o) + HALF - mine, HALF), gd_recv.at[slot, o])

    def block_piece(n, j, slot, has, needed, onward, to, step):
        @pl.when(has)
        def _():
            arrival(group_half(slot, 0, CH * j, CH), gz_recv.at[slot, j])

            @pl.when(onward)
            def _():
                send(group_half(slot, 0, CH * j, CH), group_half(slot + step, 0, CH * j, CH), gz_send.at[slot], gz_recv.at[slot + step, j], to)

            @pl.when(needed & jnp.logical_not(forwards(n)))
            def _():
                x_out(slot, j, 0, cross)

    def inner_step(n, slot):
        @pl.when(forwards(n))
        def _():
            for j in range(4):
                arrival(group_half(slot, 1, CH * j, CH), gx_recv.at[slot, j])
                x_out(slot, j, 1, inner)
            d_out(slot, 1)

    def late_step(n, slot):
        @pl.when(jnp.logical_not(forwards(n)))
        def _():
            for j in range(4):
                arrival(group_half(slot, 1, CH * j, CH), gx_recv.at[slot, j])
            d_out(slot, 1)

    def ring_cache(slot, zs, has, onward, to, step):
        @pl.when(has)
        def _():
            arrival(cache_half(0, zs), gz_recv.at[slot, 4])

            @pl.when(onward)
            def _():
                send(cache_half(0, zs), cache_half(0, zs), gz_send.at[slot], gz_recv.at[slot + step, 4], to)

            cache_cross(zs)

    def cache_cross(zs):
        @pl.when((zs + xl) % 2 == 1)
        def _():
            send(cache_half(0, zs), cache_half(1, zs), cx_send.at[zs], cx_recv.at[zs], cross)

    def cache_inner(zs):
        @pl.when((zs + xl) % 2 == 0)
        def _():
            arrival(cache_half(1, zs), cx_recv.at[zs])
            send(cache_half(1, zs), cache_half(1, zs), cx_send.at[zs], cx_recv.at[zs], inner)

    def has_up(n):
        return (n >= 1) & (n <= UP) & (z >= n)

    def has_down(n):
        return (n >= 1) & (n <= DOWN) & ((z + n) % NZ < DOWN)

    def straight(n, i):
        zs = jnp.maximum(DOWN, z + 1) + 2 * (n - 3) + i
        return zs, (n >= 3) & (zs < NZ)

    def up_needed(i):
        return (i >= 1) & (i <= UP) & (z >= i)

    def down_needed(i):
        return (i >= 1) & (i <= DOWN) & (z + i >= NZ)

    def fold_slots(first):
        for i in range(4):
            @pl.when(z > first + i)
            def _(i=i):
                d_in(first + i, 0)
                d_in(first + i, 1)

        @pl.when(z >= first + 4)
        def _():
            fold(kg, first * 256, 1024)

        @pl.when((z > first) & (z < first + 4))
        def _():
            @pl.when(z > first + 1)
            def _():
                fold(kg, first * 256, 512)

            @pl.when((z - first) % 2 == 1)
            def _():
                fold(kg, (first + (z - first) // 2 * 2) * 256, 256)

    def fold_pair(first):
        for i in range(2):
            @pl.when(z > first + i)
            def _(i=i):
                d_in(first + i, 0)
                d_in(first + i, 1)

        pl.when(z > first + 1)(lambda: fold(kg, first * 256, 512))
        pl.when(z == first + 1)(lambda: fold(kg, first * 256, 256))

    @pl.loop(1, UP + 3)
    def _(n):
        for j in range(4):
            block_piece(n, j, n - 1, has_up(n), True, (n < UP) & (z < NZ - 1), above, 1)
            block_piece(n, j, 11 - n, has_down(n), z + n >= NZ, n < DOWN, below, -1)
        ring_cache(n - 1, z - n, has_up(n), (n < UP) & (z < NZ - 1), above, 1)
        ring_cache(11 - n, (z + n) % NZ, has_down(n), n < DOWN, below, -1)
        for i in range(2):
            zs, there = straight(n, i)

            @pl.when(there)
            def _(zs=zs):
                arrival(cache_half(0, zs), cz_recv.at[zs])
                cache_cross(zs)

        pl.when(up_needed(n))(lambda: d_out(n - 1, 0))
        pl.when(down_needed(n))(lambda: d_out(11 - n, 0))
        m, p = n - 1, n - 2
        pl.when(has_up(m))(lambda: cache_inner(z - m))
        pl.when(has_down(m))(lambda: cache_inner((z + m) % NZ))
        for i in range(2):
            zs, there = straight(m, i)
            pl.when(there)(lambda zs=zs: cache_inner(zs))
        pl.when(up_needed(m))(lambda: inner_step(m, m - 1))
        pl.when(down_needed(m))(lambda: inner_step(m, 11 - m))
        pl.when(up_needed(p))(lambda: late_step(p, p - 1))
        pl.when(down_needed(p))(lambda: late_step(p, 11 - p))

        @pl.when(n == 2)
        def _():
            arrival(group_half(OWN, 1), gx_recv.at[OWN, 0])
            d_out(OWN, 1)

        @pl.when(n == UP)
        def _():
            send(cache_half(0, 0, NZ * CH), cache_half(0, 0, NZ * CH), cd_send.at[0], cd_recv.at[0], partner)

        @pl.when((n == UP - 1) | (n == UP + 1))
        def _():
            fold_pair(jnp.where(n == UP + 1, 2, 0))

    @pl.loop(0, NZ)
    def _(zs):
        @pl.when(((zs + xl) % 2 == 1) | (zs == z))
        def _():
            arrival(cache_half(1, zs), cx_recv.at[zs])

    send(cache_half(1, 0, NZ * CH), cache_half(1, 0, NZ * CH), cd_send.at[1], cd_recv.at[1], partner)
    fold_slots(4)

    for o in range(2):
        arrival(rows_at(kc, cache_row(1 - k, o, 0), NZ * CH), cd_recv.at[o])
    fold(kc, 0, 2 * NZ * CACHED)

    @pl.when(z > 8)
    def _():
        d_in(8, 0)
        d_in(8, 1)

    @pl.when(z > 9)
    def _():
        d_in(9, 0)
        d_in(9, 1)
        fold(kg, 8 * 256, 512)

    @pl.when(z == 9)
    def _():
        fold(kg, 8 * 256, 256)

    d_in(OWN, 1)

    @pl.when(z == NZ - 1)
    def _():
        d_in(10, 0)
        d_in(10, 1)
        fold(kg, 10 * 256, 512, True)

    @pl.when(z < NZ - 1)
    def _():
        fold(kg, OWN * 256, 256, True)

    loads[8].wait()
    for h in range(HEADS):
        inverse = 1.0 / l_ref[h * TOK : (h + 1) * TOK, 0:1]
        attended = (acc[h * TOK : (h + 1) * TOK, :] * inverse).astype(BF16)
        h_out[:, h * VDIM : (h + 1) * VDIM] = jnp.dot(attended, up_value[h], preferred_element_type=F32).astype(BF16)
    loads[9].wait()

    def offset_of(i):
        return jnp.where(i % 2 == 1, 4 - (i + 1) // 2, 4 + i // 2) % NY

    def window(x_side, i):
        yy = (y + offset_of(i)) % NY
        start = x_side * 3584 + yy * 448 - 64 * (yy % 2)
        cols = w[:, pl.ds(pl.multiple_of(start, 128), WIN)]
        return jnp.dot(h_out[...], cols, preferred_element_type=F32)

    LAG = 2

    def along_y(i):
        return (i == 3) | (i == 5)

    def part(ref, i, b):
        return ref.at[i, pl.ds(b * HALF, HALF), :]

    @pl.loop(0, NY + LAG)
    def _(n):
        @pl.when(n < NY)
        def _():
            sd[n] = window(1 - k, n).astype(BF16)
            send(sd.at[n], rd.at[n], rd_send.at[n], rd_recv.at[n], partner)

        @pl.when(n >= LAG)
        def _():
            i = n - LAG
            mine = window(k, i)
            arrival(rd.at[i], rd_recv.at[i])
            total = mine + rd[i].astype(F32)

            @pl.when(k == xl)
            def _():
                racc[i] = total

            @pl.when(k != xl)
            def _():
                sx[i] = total.astype(BF16)

                @pl.when((i == 5) | (i == 7))
                def _():
                    for b in range(2):
                        arrival(part(ry, i - 2, b), ry_recv.at[i - 2, b])
                    sx[i] = (total + ry[i - 2].astype(F32)).astype(BF16)

                @pl.when(along_y(i))
                def _():
                    for b in range(2):
                        send(part(sx, i, b), part(ry, i, b), ry_send.at[i], ry_recv.at[i, b], y_peer(1))

                @pl.when(jnp.logical_not(along_y(i)))
                def _():
                    for b in range(2):
                        send(part(sx, i, b), part(rx, i, b), rx_send.at[i], rx_recv.at[i, b], inner)

    @pl.when(k == xl)
    def _():
        @pl.loop(0, NY - 1)
        def _(i):
            for b in range(2):
                rows = slice(b * HALF, (b + 1) * HALF)

                @pl.when(jnp.logical_not(along_y(i)))
                def _():
                    arrival(part(rx, i, b), rx_recv.at[i, b])
                    racc[i, rows, :] = racc[i, rows, :] + rx[i, rows, :].astype(F32)

                @pl.when(i >= 2)
                def _():
                    arrival(part(ry, i - 2, b), ry_recv.at[i - 2, b])
                    racc[i, rows, :] = racc[i, rows, :] + ry[i - 2, rows, :].astype(F32)

                sy[i, rows, :] = racc[i, rows, :].astype(BF16)
                send(part(sy, i, b), part(ry, i, b), ry_send.at[i], ry_recv.at[i, b], y_peer(NY - 1 - (i % 2) * (NY - 2)))

        for b in range(2):
            arrival(part(rx, NY - 1, b), rx_recv.at[NY - 1, b])
        racc[NY - 1] = racc[NY - 1] + rx[NY - 1].astype(F32)
        for i in (NY - 3, NY - 2):
            for b in range(2):
                arrival(part(ry, i, b), ry_recv.at[i, b])
            racc[NY - 1] = racc[NY - 1] + ry[i].astype(F32)
        total_t[...] = racc[NY - 1].T
        sf[...] = total_t[pl.ds(pl.multiple_of(64 * (y % 2) + 224 * (1 - k), 32), 224), :].astype(BF16)
        send(sf, rf, rf_send.at[0], rf_recv.at[0], partner)
        out_ref[...] = total_t[pl.ds(pl.multiple_of(64 * (y % 2) + 224 * k, 32), 224), :].astype(BF16)

    @pl.when(k != xl)
    def _():
        arrival(rf, rf_recv.at[0])
        out_ref[...] = rf[...]

    half_rows = rows_at(kg, 0, HALF)
    block_rows = rows_at(kg, 0, HALF + CH)
    pl.when(z < NZ - 1)(lambda: sent(block_rows, gz_send.at[11]))
    pl.when(z < DOWN)(lambda: sent(block_rows, gz_send.at[12]))
    sent(half_rows, gx_send.at[OWN])
    sent(half_rows, gd_send.at[OWN, 1])

    @pl.loop(1, UP + 1)
    def _(n):
        pl.when((n < UP) & (z < NZ - 1) & has_up(n))(lambda: sent(block_rows, gz_send.at[n - 1]))
        pl.when((n < DOWN) & has_down(n))(lambda: sent(block_rows, gz_send.at[11 - n]))

    @pl.loop(0, z)
    def _(i):
        sent(half_rows, gx_send.at[i])
        sent(half_rows, gd_send.at[i, 0])
        sent(half_rows, gd_send.at[i, 1])

    @pl.loop(0, NZ)
    def _(i):
        sent(rows_at(kc, 0, CH), cx_send.at[i])
        pl.when((z >= DOWN) & (i < z))(lambda: sent(rows_at(kc, 0, CH), cz_send.at[i]))

    for o in range(2):
        sent(rows_at(kc, 0, NZ * CH), cd_send.at[o])

    @pl.loop(0, NY)
    def _(i):
        sent(sd.at[i], rd_send.at[i])

    @pl.when(k != xl)
    def _():
        @pl.loop(0, NY)
        def _(i):
            pl.when(jnp.logical_not(along_y(i)))(lambda: sent(sx.at[i], rx_send.at[i]))
            pl.when(along_y(i))(lambda: sent(sx.at[i], ry_send.at[i]))

    @pl.when(k == xl)
    def _():
        @pl.loop(0, NY - 1)
        def _(i):
            sent(sy.at[i], ry_send.at[i])

        sent(sf, rf_send.at[0])


def local(q_nope, q_rope, cache_latent, group_latent, offset, counts, up_key, up_value, out_weight):
    k32 = np.arange(128) % 32
    freq = jnp.asarray((10000.0 ** (-2.0 * k32 / ROPE)).astype(np.float32)[None, :])
    any_spec = pl.BlockSpec(memory_space=pl.ANY)
    vmem = pl.BlockSpec(memory_space=pltpu.VMEM)
    dma = pltpu.SemaphoreType.DMA
    win = (TOK, WIN)
    return pl.pallas_call(
        kernel,
        out_shape=jax.ShapeDtypeStruct((224, TOK), BF16),
        in_specs=[any_spec] * 10,
        out_specs=vmem,
        scratch_shapes=[
            pltpu.SMEM((1,), jnp.int32),
            pltpu.SMEM((24,), jnp.int32),
            pltpu.VMEM((1, 128), F32),
            pltpu.VMEM((TOK, HEADS * NOPE), BF16),
            pltpu.VMEM((TOK, HEADS * ROPE), BF16),
            pltpu.VMEM((CACHED, LATENT + ROPE), BF16),
            pltpu.VMEM((LATENT + ROPE, TOK), BF16),
            pltpu.VMEM((HEADS, NOPE, LATENT), BF16),
            pltpu.VMEM((HEADS, LATENT, VDIM), BF16),
            pltpu.VMEM((HEADS * VDIM, 7168), BF16),
            pltpu.VMEM((12 * 256, WIDE), BF16),
            pltpu.VMEM((2 * NZ * CACHED, WIDE), BF16),
            pltpu.VMEM((ROWS, WIDE), BF16),
            pltpu.VMEM((ROWS, LATENT), F32),
            pltpu.VMEM((ROWS, 128), F32),
            pltpu.VMEM((ROWS, 128), F32),
            pltpu.VMEM((TOK, HEADS * VDIM), BF16),
            pltpu.VMEM((NY, *win), BF16),
            pltpu.VMEM((NY, *win), BF16),
            pltpu.VMEM((NY, *win), BF16),
            pltpu.VMEM((NY, *win), BF16),
            pltpu.VMEM((NY, *win), F32),
            pltpu.VMEM((NY - 1, *win), BF16),
            pltpu.VMEM((NY - 1, *win), BF16),
            pltpu.VMEM((224, TOK), BF16),
            pltpu.VMEM((224, TOK), BF16),
            pltpu.VMEM((WIN, TOK), F32),
            dma((10,)), dma((13,)), dma((11, 5)), dma((12,)), dma((12, 4)), dma((12, 2)), dma((12, 2)),
            dma((12,)), dma((12,)), dma((12,)), dma((12,)), dma((2,)), dma((2,)),
            dma((NY,)), dma((NY,)), dma((NY,)), dma((NY, 2)), dma((NY - 1,)), dma((NY - 1, 2)), dma((1,)), dma((1,)),
        ],
        compiler_params=pltpu.CompilerParams(collective_id=0, has_side_effects=True, vmem_limit_bytes=60000 * 1024),
    )(offset, counts, freq, q_nope, q_rope, cache_latent, group_latent.T, up_key, up_value, out_weight).T


def solution(mesh):
    in_specs = (
        P("ctx", "tp"), P("ctx", "tp"), P("ctx", None), P("ctx", None), P(), P(),
        P("tp", None, None), P("tp", None, None), P("tp", None),
    )
    return jax.shard_map(local, mesh=mesh, in_specs=in_specs, out_specs=P("ctx", "tp"), check_vma=False)
```

```python
import math

import jax
import jax.numpy as jnp
import numpy as np
from jax import lax
from jax.experimental import pallas as pl
from jax.experimental.pallas import tpu as pltpu
from jax.sharding import PartitionSpec as P

LATENT = 512
ROPE = 64
NOPE = 128
VDIM = 128
WIDE = 640
NZ = 12
NY = 8
TOK = 128
CACHED = 32
HEADS = 4
ROWS = TOK * HEADS
UP = 6
DOWN = 5
OWN = 11
HALF = 64
CH = 16
WIN = 512
NEG = -1e30
SCALE = math.log2(math.e) / math.sqrt(NOPE + ROPE)
GROUP = 256
MESH = pl.DeviceIdType.MESH
F32 = jnp.float32
BF16 = jnp.bfloat16


def group_row(slot, o):
    return slot * 256 + o * TOK


def cache_row(half, o, zs):
    return ((half * 2 + o) * NZ + zs) * CH


def rows_at(ref, start, size):
    if not isinstance(start, int):
        start = pl.multiple_of(start, 16)
    return ref.at[pl.ds(start, size), :]


def kernel(
    offset_hbm, counts_hbm, freq_hbm, q_nope_hbm, q_rope_hbm, cache_hbm, group_hbm, up_key_hbm, up_value_hbm, w_hbm,
    out_ref,
    offset_ref, counts_ref, freq_ref, q_nope, q_rope, cache, group, up_key, up_value, w,
    kg, kc, q, acc, m_ref, l_ref, h_out,
    sd, rd, sx, rx, racc, sy, ry, sf, rf, total_t,
    in_sem, gz_send, gz_recv, gx_send, gx_recv, gd_send, gd_recv, cz_send, cz_recv, cx_send, cx_recv, cd_send, cd_recv,
    rd_send, rd_recv, rx_send, rx_recv, ry_send, ry_recv, rf_send, rf_recv,
):
    c = lax.axis_index("ctx")
    t = lax.axis_index("tp")
    z, xh = c // 2, c % 2
    xl, y, k = t // 16, (t // 2) % 8, t % 2

    def dev(cc, tt):
        return (cc, tt)

    above = dev(((z + 1) % NZ) * 2 + xh, t)
    below = dev(((z + NZ - 1) % NZ) * 2 + xh, t)
    cross = dev(z * 2 + 1 - xh, (1 - xl) * 16 + y * 2 + k)
    inner = dev(c, (1 - xl) * 16 + y * 2 + k)
    partner = dev(c, xl * 16 + y * 2 + 1 - k)

    def y_peer(o):
        return dev(c, xl * 16 + ((y + o) % NY) * 2 + k)

    loads = [
        pltpu.make_async_copy(src, dst, in_sem.at[i])
        for i, (src, dst) in enumerate(
            [(group_hbm, group), (cache_hbm, cache), (offset_hbm, offset_ref), (counts_hbm, counts_ref), (freq_hbm, freq_ref), (q_nope_hbm, q_nope), (up_key_hbm, up_key), (q_rope_hbm, q_rope),
             (up_value_hbm, up_value), (w_hbm, w)]
        )
    ]
    for load in loads:
        load.start()

    barrier = pltpu.get_barrier_semaphore()
    for peer in [below, above, cross, inner, partner, y_peer(1), y_peer(NY - 1)]:
        pl.semaphore_signal(barrier, inc=1, device_id=peer, device_id_type=MESH)

    @pl.loop(jnp.maximum(DOWN, z + 2), jnp.where(z == 0, NZ - 1, NZ))
    def _(zh):
        pl.semaphore_signal(barrier, inc=1, device_id=dev(zh * 2 + xh, t), device_id_type=MESH)

    for i in (2, 3, 4):
        loads[i].wait()

    lane = lax.broadcasted_iota(jnp.int32, (TOK, 128), 1)
    row = lax.broadcasted_iota(jnp.int32, (TOK, 128), 0)
    angles = (offset_ref[0] + c * TOK + row).astype(F32) * freq_ref[...]
    cosine, sine = jnp.cos(angles), jnp.sin(angles)
    sine = jnp.where(lane % 64 < 32, -sine, sine)

    def rotate(v):
        other = jnp.where(lane % 64 < 32, pltpu.roll(v, 96, 1), pltpu.roll(v, 32, 1))
        return v * cosine + other * sine

    own = group_row(OWN, 0)
    loads[0].wait()
    loads[1].wait()
    lane16 = lane[0:CH]
    rows, into = pl.ds(pl.multiple_of(CH * k, CH), CH), pl.ds(pl.multiple_of(cache_row(k, 0, z), CH), CH)
    dead = jnp.where((lane16 == 64) & (row[0:CH] + CH * k >= counts_ref[c]), 1.0, 0.0)
    held = cache[rows, LATENT : LATENT + ROPE].astype(F32)
    held = jnp.concatenate([held, held], 1)
    kc[into, 0:LATENT] = cache[rows, 0:LATENT]
    kc[into, LATENT:WIDE] = jnp.where(lane16 < 64, held, dead).astype(BF16)
    for part in range(LATENT // 128):
        cols = slice(part * 128, (part + 1) * 128)
        kg[own : own + TOK, cols] = group[cols, :].T
    tail = group[LATENT : LATENT + ROPE, :].astype(F32)
    tail = rotate(jnp.concatenate([tail, tail], 0).T)
    owned = jnp.where(lane == 65 + c, 1.0, 0.0)
    kg[own : own + TOK, LATENT:WIDE] = jnp.where(lane < 64, tail, owned).astype(BF16)

    pl.semaphore_wait(barrier, 7 + jnp.where(z >= DOWN, z - 1 - z // (NZ - 1), 0))

    def send(src, dst, s_sem, r_sem, to):
        pltpu.make_async_remote_copy(src_ref=src, dst_ref=dst, send_sem=s_sem, recv_sem=r_sem, device_id=to, device_id_type=MESH).start()

    def arrival(view, r_sem):
        pltpu.make_async_remote_copy(src_ref=view, dst_ref=view, send_sem=r_sem, recv_sem=r_sem, device_id=partner, device_id_type=MESH).wait_recv()

    def sent(view, s_sem):
        pltpu.make_async_remote_copy(src_ref=view, dst_ref=view, send_sem=s_sem, recv_sem=s_sem, device_id=partner, device_id_type=MESH).wait_send()

    mine = HALF * k

    def group_half(slot, o, r=0, size=HALF):
        return rows_at(kg, group_row(slot, o) + mine + r, size)

    def cache_half(o, zs, size=CH):
        return rows_at(kc, cache_row(k, o, zs), size)

    def first_send(slot, s_sem, to):
        for j in range(4):
            send(group_half(OWN, 0, CH * j, CH), group_half(slot, 0, CH * j, CH), s_sem, gz_recv.at[slot, j], to)
        send(cache_half(0, z), cache_half(0, z), s_sem, gz_recv.at[slot, 4], to)

    pl.when(z < NZ - 1)(lambda: first_send(0, gz_send.at[11], above))
    pl.when(z < DOWN)(lambda: first_send(10, gz_send.at[12], below))

    @pl.when(z >= DOWN)
    def _():
        @pl.loop(0, z)
        def _(zl):
            send(cache_half(0, z), cache_half(0, z), cz_send.at[zl], cz_recv.at[z], dev(zl * 2 + xh, t))

    send(cache_half(0, z), cache_half(1, z), cx_send.at[z], cx_recv.at[z], cross)
    send(group_half(OWN, 0), group_half(OWN, 1), gx_send.at[OWN], gx_recv.at[OWN, 0], cross)

    loads[5].wait()
    loads[6].wait()
    loads[7].wait()
    for h in range(HEADS):
        lat = jnp.dot(q_nope[:, h * NOPE : (h + 1) * NOPE], up_key[h], preferred_element_type=F32)
        q[h * TOK : (h + 1) * TOK, 0:LATENT] = (lat * SCALE).astype(BF16)
    hides = jnp.where((lane == 64) | ((lane > 65 + c) & (lane < 65 + 24)), NEG, 0.0)
    for pair in range(HEADS // 2):
        turned = rotate(q_rope[:, pair * 128 : (pair + 1) * 128].astype(F32)) * SCALE
        for part in range(2):
            moved = turned if part == 0 else pltpu.roll(turned, 64, 1)
            h = 2 * pair + part
            q[h * TOK : (h + 1) * TOK, LATENT:WIDE] = jnp.where(lane < 64, moved, hides).astype(BF16)
    m_ref[...] = jnp.full(m_ref.shape, NEG, F32)
    l_ref[...] = jnp.zeros(l_ref.shape, F32)
    acc[...] = jnp.zeros(acc.shape, F32)

    def fold(ref, base, size, last=False):
        for g in range(ROWS // GROUP):
            r = slice(g * GROUP, (g + 1) * GROUP)
            keys = rows_at(ref, base, size)[...]
            s = lax.dot_general(q[r, :], keys, (((1,), (1,)), ((), ())), preferred_element_type=F32)
            if last:
                token = lax.broadcasted_iota(jnp.int32, (GROUP, TOK), 0) % TOK
                key = lax.broadcasted_iota(jnp.int32, (GROUP, TOK), 1)
                masked = jnp.where(key > token, NEG, s[:, size - 256 : size - TOK])
                s = jnp.concatenate([s[:, 0 : size - 256], masked, s[:, size - TOK :]], 1) if size > 256 else jnp.concatenate([masked, s[:, TOK:]], 1)
            old = m_ref[r, 0:1]
            top = jnp.maximum(old, jnp.max(s, axis=1, keepdims=True))
            alpha = jnp.exp2(old - top)
            e = jnp.exp2(s - top)
            total = jnp.sum(e, axis=1, keepdims=True) + l_ref[r, 0:1] * alpha
            mixed = jnp.dot(e.astype(BF16), keys[:, 0:LATENT], preferred_element_type=F32) + acc[r, :] * alpha
            m_ref[r, :] = jnp.broadcast_to(top, (GROUP, 128))
            l_ref[r, :] = jnp.broadcast_to(total, (GROUP, 128))
            acc[r, :] = mixed

    def forwards(i):
        return (z + i + xl + k) % 2 == 0

    def x_out(slot, j, o, to):
        send(group_half(slot, o, CH * j, CH), group_half(slot, 1, CH * j, CH), gx_send.at[slot], gx_recv.at[slot, j], to)

    def d_out(slot, o):
        send(group_half(slot, o), group_half(slot, o), gd_send.at[slot, o], gd_recv.at[slot, o], partner)

    def d_in(slot, o):
        arrival(rows_at(kg, group_row(slot, o) + HALF - mine, HALF), gd_recv.at[slot, o])

    def block_piece(n, j, slot, has, needed, onward, to, step):
        @pl.when(has)
        def _():
            arrival(group_half(slot, 0, CH * j, CH), gz_recv.at[slot, j])

            @pl.when(onward)
            def _():
                send(group_half(slot, 0, CH * j, CH), group_half(slot + step, 0, CH * j, CH), gz_send.at[slot], gz_recv.at[slot + step, j], to)

            @pl.when(needed & jnp.logical_not(forwards(n)))
            def _():
                x_out(slot, j, 0, cross)

    def inner_step(n, slot):
        @pl.when(forwards(n))
        def _():
            for j in range(4):
                arrival(group_half(slot, 1, CH * j, CH), gx_recv.at[slot, j])
                x_out(slot, j, 1, inner)
            d_out(slot, 1)

    def late_step(n, slot):
        @pl.when(jnp.logical_not(forwards(n)))
        def _():
            for j in range(4):
                arrival(group_half(slot, 1, CH * j, CH), gx_recv.at[slot, j])
            d_out(slot, 1)

    def ring_cache(slot, zs, has, onward, to, step):
        @pl.when(has)
        def _():
            arrival(cache_half(0, zs), gz_recv.at[slot, 4])

            @pl.when(onward)
            def _():
                send(cache_half(0, zs), cache_half(0, zs), gz_send.at[slot], gz_recv.at[slot + step, 4], to)

            cache_cross(zs)

    def cache_cross(zs):
        @pl.when((zs + xl) % 2 == 1)
        def _():
            send(cache_half(0, zs), cache_half(1, zs), cx_send.at[zs], cx_recv.at[zs], cross)

    def cache_inner(zs):
        @pl.when((zs + xl) % 2 == 0)
        def _():
            arrival(cache_half(1, zs), cx_recv.at[zs])
            send(cache_half(1, zs), cache_half(1, zs), cx_send.at[zs], cx_recv.at[zs], inner)

    def has_up(n):
        return (n >= 1) & (n <= UP) & (z >= n)

    def has_down(n):
        return (n >= 1) & (n <= DOWN) & ((z + n) % NZ < DOWN)

    def straight(n, i):
        zs = jnp.maximum(DOWN, z + 1) + 2 * (n - 3) + i
        return zs, (n >= 3) & (zs < NZ)

    def up_needed(i):
        return (i >= 1) & (i <= UP) & (z >= i)

    def down_needed(i):
        return (i >= 1) & (i <= DOWN) & (z + i >= NZ)

    def fold_slots(first):
        for i in range(4):
            @pl.when(z > first + i)
            def _(i=i):
                d_in(first + i, 0)
                d_in(first + i, 1)

        @pl.when(z >= first + 4)
        def _():
            fold(kg, first * 256, 1024)

        @pl.when((z > first) & (z < first + 4))
        def _():
            @pl.when(z > first + 1)
            def _():
                fold(kg, first * 256, 512)

            @pl.when((z - first) % 2 == 1)
            def _():
                fold(kg, (first + (z - first) // 2 * 2) * 256, 256)

    @pl.loop(1, UP + 3)
    def _(n):
        for j in range(4):
            block_piece(n, j, n - 1, has_up(n), True, (n < UP) & (z < NZ - 1), above, 1)
            block_piece(n, j, 11 - n, has_down(n), z + n >= NZ, n < DOWN, below, -1)
        ring_cache(n - 1, z - n, has_up(n), (n < UP) & (z < NZ - 1), above, 1)
        ring_cache(11 - n, (z + n) % NZ, has_down(n), n < DOWN, below, -1)
        for i in range(2):
            zs, there = straight(n, i)

            @pl.when(there)
            def _(zs=zs):
                arrival(cache_half(0, zs), cz_recv.at[zs])
                cache_cross(zs)

        pl.when(up_needed(n))(lambda: d_out(n - 1, 0))
        pl.when(down_needed(n))(lambda: d_out(11 - n, 0))
        m, p = n - 1, n - 2
        pl.when(has_up(m))(lambda: cache_inner(z - m))
        pl.when(has_down(m))(lambda: cache_inner((z + m) % NZ))
        for i in range(2):
            zs, there = straight(m, i)
            pl.when(there)(lambda zs=zs: cache_inner(zs))
        pl.when(up_needed(m))(lambda: inner_step(m, m - 1))
        pl.when(down_needed(m))(lambda: inner_step(m, 11 - m))
        pl.when(up_needed(p))(lambda: late_step(p, p - 1))
        pl.when(down_needed(p))(lambda: late_step(p, 11 - p))

        @pl.when(n == 2)
        def _():
            arrival(group_half(OWN, 1), gx_recv.at[OWN, 0])
            d_out(OWN, 1)

        @pl.when(n == UP)
        def _():
            send(cache_half(0, 0, NZ * CH), cache_half(0, 0, NZ * CH), cd_send.at[0], cd_recv.at[0], partner)

        @pl.when(n == UP + 1)
        def _():
            fold_slots(0)

    @pl.loop(0, NZ)
    def _(zs):
        @pl.when(((zs + xl) % 2 == 1) | (zs == z))
        def _():
            arrival(cache_half(1, zs), cx_recv.at[zs])

    send(cache_half(1, 0, NZ * CH), cache_half(1, 0, NZ * CH), cd_send.at[1], cd_recv.at[1], partner)
    fold_slots(4)

    for o in range(2):
        arrival(rows_at(kc, cache_row(1 - k, o, 0), NZ * CH), cd_recv.at[o])
    fold(kc, 0, 2 * NZ * CACHED)

    @pl.when(z > 8)
    def _():
        d_in(8, 0)
        d_in(8, 1)

    @pl.when(z > 9)
    def _():
        d_in(9, 0)
        d_in(9, 1)
        fold(kg, 8 * 256, 512)

    @pl.when(z == 9)
    def _():
        fold(kg, 8 * 256, 256)

    d_in(OWN, 1)

    @pl.when(z == NZ - 1)
    def _():
        d_in(10, 0)
        d_in(10, 1)
        fold(kg, 10 * 256, 512, True)

    @pl.when(z < NZ - 1)
    def _():
        fold(kg, OWN * 256, 256, True)

    loads[8].wait()
    for h in range(HEADS):
        inverse = 1.0 / l_ref[h * TOK : (h + 1) * TOK, 0:1]
        attended = (acc[h * TOK : (h + 1) * TOK, :] * inverse).astype(BF16)
        h_out[:, h * VDIM : (h + 1) * VDIM] = jnp.dot(attended, up_value[h], preferred_element_type=F32).astype(BF16)
    loads[9].wait()

    def offset_of(i):
        return jnp.where(i % 2 == 1, 4 - (i + 1) // 2, 4 + i // 2) % NY

    def window(x_side, i):
        yy = (y + offset_of(i)) % NY
        start = x_side * 3584 + yy * 448 - 64 * (yy % 2)
        cols = w[:, pl.ds(pl.multiple_of(start, 128), WIN)]
        return jnp.dot(h_out[...], cols, preferred_element_type=F32)

    LAG = 2

    def along_y(i):
        return (i == 3) | (i == 5)

    def part(ref, i, b):
        return ref.at[i, pl.ds(b * HALF, HALF), :]

    @pl.loop(0, NY + LAG)
    def _(n):
        @pl.when(n < NY)
        def _():
            sd[n] = window(1 - k, n).astype(BF16)
            send(sd.at[n], rd.at[n], rd_send.at[n], rd_recv.at[n], partner)

        @pl.when(n >= LAG)
        def _():
            i = n - LAG
            mine = window(k, i)
            arrival(rd.at[i], rd_recv.at[i])
            total = mine + rd[i].astype(F32)

            @pl.when(k == xl)
            def _():
                racc[i] = total

            @pl.when(k != xl)
            def _():
                sx[i] = total.astype(BF16)

                @pl.when((i == 5) | (i == 7))
                def _():
                    for b in range(2):
                        arrival(part(ry, i - 2, b), ry_recv.at[i - 2, b])
                    sx[i] = (total + ry[i - 2].astype(F32)).astype(BF16)

                @pl.when(along_y(i))
                def _():
                    for b in range(2):
                        send(part(sx, i, b), part(ry, i, b), ry_send.at[i], ry_recv.at[i, b], y_peer(1))

                @pl.when(jnp.logical_not(along_y(i)))
                def _():
                    for b in range(2):
                        send(part(sx, i, b), part(rx, i, b), rx_send.at[i], rx_recv.at[i, b], inner)

    @pl.when(k == xl)
    def _():
        @pl.loop(0, NY - 1)
        def _(i):
            for b in range(2):
                rows = slice(b * HALF, (b + 1) * HALF)

                @pl.when(jnp.logical_not(along_y(i)))
                def _():
                    arrival(part(rx, i, b), rx_recv.at[i, b])
                    racc[i, rows, :] = racc[i, rows, :] + rx[i, rows, :].astype(F32)

                @pl.when(i >= 2)
                def _():
                    arrival(part(ry, i - 2, b), ry_recv.at[i - 2, b])
                    racc[i, rows, :] = racc[i, rows, :] + ry[i - 2, rows, :].astype(F32)

                sy[i, rows, :] = racc[i, rows, :].astype(BF16)
                send(part(sy, i, b), part(ry, i, b), ry_send.at[i], ry_recv.at[i, b], y_peer(NY - 1 - (i % 2) * (NY - 2)))

        for b in range(2):
            arrival(part(rx, NY - 1, b), rx_recv.at[NY - 1, b])
        racc[NY - 1] = racc[NY - 1] + rx[NY - 1].astype(F32)
        for i in (NY - 3, NY - 2):
            for b in range(2):
                arrival(part(ry, i, b), ry_recv.at[i, b])
            racc[NY - 1] = racc[NY - 1] + ry[i].astype(F32)
        total_t[...] = racc[NY - 1].T
        sf[...] = total_t[pl.ds(pl.multiple_of(64 * (y % 2) + 224 * (1 - k), 32), 224), :].astype(BF16)
        send(sf, rf, rf_send.at[0], rf_recv.at[0], partner)
        out_ref[...] = total_t[pl.ds(pl.multiple_of(64 * (y % 2) + 224 * k, 32), 224), :].astype(BF16)

    @pl.when(k != xl)
    def _():
        arrival(rf, rf_recv.at[0])
        out_ref[...] = rf[...]

    half_rows = rows_at(kg, 0, HALF)
    block_rows = rows_at(kg, 0, HALF + CH)
    pl.when(z < NZ - 1)(lambda: sent(block_rows, gz_send.at[11]))
    pl.when(z < DOWN)(lambda: sent(block_rows, gz_send.at[12]))
    sent(half_rows, gx_send.at[OWN])
    sent(half_rows, gd_send.at[OWN, 1])

    @pl.loop(1, UP + 1)
    def _(n):
        pl.when((n < UP) & (z < NZ - 1) & has_up(n))(lambda: sent(block_rows, gz_send.at[n - 1]))
        pl.when((n < DOWN) & has_down(n))(lambda: sent(block_rows, gz_send.at[11 - n]))

    @pl.loop(0, z)
    def _(i):
        sent(half_rows, gx_send.at[i])
        sent(half_rows, gd_send.at[i, 0])
        sent(half_rows, gd_send.at[i, 1])

    @pl.loop(0, NZ)
    def _(i):
        sent(rows_at(kc, 0, CH), cx_send.at[i])
        pl.when((z >= DOWN) & (i < z))(lambda: sent(rows_at(kc, 0, CH), cz_send.at[i]))

    for o in range(2):
        sent(rows_at(kc, 0, NZ * CH), cd_send.at[o])

    @pl.loop(0, NY)
    def _(i):
        sent(sd.at[i], rd_send.at[i])

    @pl.when(k != xl)
    def _():
        @pl.loop(0, NY)
        def _(i):
            pl.when(jnp.logical_not(along_y(i)))(lambda: sent(sx.at[i], rx_send.at[i]))
            pl.when(along_y(i))(lambda: sent(sx.at[i], ry_send.at[i]))

    @pl.when(k == xl)
    def _():
        @pl.loop(0, NY - 1)
        def _(i):
            sent(sy.at[i], ry_send.at[i])

        sent(sf, rf_send.at[0])


def local(q_nope, q_rope, cache_latent, group_latent, offset, counts, up_key, up_value, out_weight):
    k32 = np.arange(128) % 32
    freq = jnp.asarray((10000.0 ** (-2.0 * k32 / ROPE)).astype(np.float32)[None, :])
    any_spec = pl.BlockSpec(memory_space=pl.ANY)
    vmem = pl.BlockSpec(memory_space=pltpu.VMEM)
    dma = pltpu.SemaphoreType.DMA
    win = (TOK, WIN)
    return pl.pallas_call(
        kernel,
        out_shape=jax.ShapeDtypeStruct((224, TOK), BF16),
        in_specs=[any_spec] * 10,
        out_specs=vmem,
        scratch_shapes=[
            pltpu.SMEM((1,), jnp.int32),
            pltpu.SMEM((24,), jnp.int32),
            pltpu.VMEM((1, 128), F32),
            pltpu.VMEM((TOK, HEADS * NOPE), BF16),
            pltpu.VMEM((TOK, HEADS * ROPE), BF16),
            pltpu.VMEM((CACHED, LATENT + ROPE), BF16),
            pltpu.VMEM((LATENT + ROPE, TOK), BF16),
            pltpu.VMEM((HEADS, NOPE, LATENT), BF16),
            pltpu.VMEM((HEADS, LATENT, VDIM), BF16),
            pltpu.VMEM((HEADS * VDIM, 7168), BF16),
            pltpu.VMEM((12 * 256, WIDE), BF16),
            pltpu.VMEM((2 * NZ * CACHED, WIDE), BF16),
            pltpu.VMEM((ROWS, WIDE), BF16),
            pltpu.VMEM((ROWS, LATENT), F32),
            pltpu.VMEM((ROWS, 128), F32),
            pltpu.VMEM((ROWS, 128), F32),
            pltpu.VMEM((TOK, HEADS * VDIM), BF16),
            pltpu.VMEM((NY, *win), BF16),
            pltpu.VMEM((NY, *win), BF16),
            pltpu.VMEM((NY, *win), BF16),
            pltpu.VMEM((NY, *win), BF16),
            pltpu.VMEM((NY, *win), F32),
            pltpu.VMEM((NY - 1, *win), BF16),
            pltpu.VMEM((NY - 1, *win), BF16),
            pltpu.VMEM((224, TOK), BF16),
            pltpu.VMEM((224, TOK), BF16),
            pltpu.VMEM((WIN, TOK), F32),
            dma((10,)), dma((13,)), dma((11, 5)), dma((12,)), dma((12, 4)), dma((12, 2)), dma((12, 2)),
            dma((12,)), dma((12,)), dma((12,)), dma((12,)), dma((2,)), dma((2,)),
            dma((NY,)), dma((NY,)), dma((NY,)), dma((NY, 2)), dma((NY - 1,)), dma((NY - 1, 2)), dma((1,)), dma((1,)),
        ],
        compiler_params=pltpu.CompilerParams(collective_id=0, has_side_effects=True, vmem_limit_bytes=60000 * 1024),
    )(offset, counts, freq, q_nope, q_rope, cache_latent, group_latent.T, up_key, up_value, out_weight).T


def solution(mesh):
    in_specs = (
        P("ctx", "tp"), P("ctx", "tp"), P("ctx", None), P("ctx", None), P(), P(),
        P("tp", None, None), P("tp", None, None), P("tp", None),
    )
    return jax.shard_map(local, mesh=mesh, in_specs=in_specs, out_specs=P("ctx", "tp"), check_vma=False)
```
